8 devices in a mesh: data: 1 (over z), store: 2 (over y), model: 4 (over x, core).
Axes of the slice: x: 2, y: 2, z: 1, core: 2. Of those that a mesh axis runs over, the one named last changes fastest.
Arguments:
- queries: bfloat16 [128, 2560], P('data')
- w_head: bfloat16 [2560, 51200], P(None, 'model')
- store_keys: bfloat16 [131072, 2560], P(('store', 'model'))
- store_tok: int32 [131072], P(('store', 'model'))
- temperature: float32 [], replicated
- mix_weight: float32 [], replicated
Outputs:
- output: float32 [128, 51200], P(('data', 'store'), 'model')
All inputs are finite; a program needn't handle non-finite values.
Results may differ from the reference program's by a relative error of at most 0.001.
Values are sent between devices in bfloat16 or wider.
A program may use at most 1 GiB of HBM per device.

```python
import jax
import jax.numpy as jnp
from jax import lax

HIDDEN = 2560
VOCAB = 51200
ROWS_DEV = 64
KEYS_DEV = 16384
STORE_DEVS = 2
MODEL_DEVS = 4
BATCH = ROWS_DEV * STORE_DEVS
SHARDS = STORE_DEVS * MODEL_DEVS
N_KEYS = KEYS_DEV * SHARDS


def setup_inputs(seed: int = 0, part: int = 0) -> dict:
    base_key = jax.random.key(seed)
    part_key = jax.random.fold_in(base_key, part)
    key_head, key_store, key_tok_a, key_tok_b, key_temp, key_mix = jax.random.split(base_key, 6)
    queries = jax.random.normal(part_key, (BATCH, HIDDEN), jnp.float32)
    w_head = jax.random.normal(key_head, (HIDDEN, VOCAB), jnp.float32) * HIDDEN ** -0.5
    store_keys = jax.random.normal(key_store, (N_KEYS, HIDDEN), jnp.float32)
    tok_a = jax.random.randint(key_tok_a, (N_KEYS,), 0, VOCAB, jnp.int32)
    tok_b = jax.random.randint(key_tok_b, (N_KEYS,), 0, VOCAB, jnp.int32)
    store_tok = jnp.minimum(tok_a, tok_b).at[0].set(0).at[N_KEYS - 1].set(VOCAB - 1)
    temperature = (6.0 * HIDDEN) ** 0.5 / 1.5 * jax.random.uniform(key_temp, (), jnp.float32, minval=0.6, maxval=1.5)
    mix_weight = jax.random.uniform(key_mix, (), jnp.float32, minval=0.25, maxval=0.5)
    return {"queries": queries.astype(jnp.bfloat16), "w_head": w_head.astype(jnp.bfloat16), "store_keys": store_keys.astype(jnp.bfloat16), "store_tok": store_tok, "temperature": temperature, "mix_weight": mix_weight}


def reference(queries, w_head, store_keys, store_tok, temperature, mix_weight):
    key_blocks = store_keys.reshape(SHARDS, KEYS_DEV, HIDDEN)
    tok_blocks = store_tok.reshape(SHARDS, KEYS_DEV)

    def block_scores(block):
        key_dots = jnp.dot(block, queries.T, preferred_element_type=jnp.float32)
        key_norms = jnp.sum(jnp.square(block.astype(jnp.float32)), axis=1)
        return (2.0 * key_dots - key_norms[:, None]) / temperature

    block_top = lax.map(lambda block: jnp.max(block_scores(block), axis=0), key_blocks)
    row_top = jnp.max(block_top, axis=0)

    def accumulate(carry, pair):
        histogram, row_total = carry
        block, tok_ids = pair
        weights = jnp.exp(block_scores(block) - row_top)
        histogram = histogram + jax.ops.segment_sum(weights, tok_ids, num_segments=VOCAB)
        row_total = row_total + jnp.sum(weights, axis=0)
        return (histogram, row_total), None

    init_state = (jnp.zeros((VOCAB, BATCH), jnp.float32), jnp.zeros((BATCH,), jnp.float32))
    (histogram, row_total), _ = lax.scan(accumulate, init_state, (key_blocks, tok_blocks))
    knn_prob = (histogram / row_total).T
    logits = jnp.dot(queries, w_head, preferred_element_type=jnp.float32)
    lm_exp = jnp.exp(logits - jnp.max(logits, axis=1, keepdims=True))
    lm_prob = lm_exp / jnp.sum(lm_exp, axis=1, keepdims=True)
    return jnp.log(mix_weight * knn_prob + (1.0 - mix_weight) * lm_prob)
```

```python
import functools

import jax
import jax.numpy as jnp
from jax import lax
from jax.experimental import pallas as pl
from jax.experimental.pallas import tpu as pltpu
from jax.sharding import PartitionSpec as P

F32 = jnp.float32
ANY = pl.ANY
VMEM = pltpu.VMEM
SMEM = pltpu.SMEM
KEY_BLOCK = 512
BATCH_KEYS = 16
FLAG_KEYS = 64
PACK = 4
TOK_BLOCK = 128
STAGE_BLOCKS = 5
HEAD = 8


def lane_group(width):
    return lax.broadcasted_iota(jnp.int32, (1, 128), 1) // width


def pick(group, parts):
    out = parts[-1]
    for index in range(len(parts) - 2, -1, -1):
        out = jnp.where(group == index, parts[index], out)
    return out


def roll(value, shift):
    return pltpu.roll(value, shift % 128, 1)


def score_kernel(tau_ref, q_ref, k_ref, own_ref, first_ref, second_ref):
    tau = tau_ref[0]
    dots = jnp.dot(k_ref[...], q_ref[...], preferred_element_type=F32)
    step = 128
    norms = []
    for row in range(0, KEY_BLOCK, step):
        acc = jnp.zeros((step, 128), F32)
        for col in range(0, k_ref.shape[1], 128):
            part = k_ref[row : row + step, col : col + 128].astype(F32)
            acc += part * part
        norms.append(jnp.sum(acc, axis=1, keepdims=True))
    group = lane_group(32)
    scores = [(2.0 * dots[i * step : (i + 1) * step] - norms[i]) / tau for i in range(KEY_BLOCK // step)]
    for i in range(KEY_BLOCK // step // 2):
        own_ref[i * step : (i + 1) * step, :] = jnp.where(group < 2, scores[2 * i], roll(scores[2 * i + 1], 64))
    for i in range(KEY_BLOCK // step // 4):
        four = scores[4 * i : 4 * i + 4]
        rows = slice(i * step, (i + 1) * step)
        first_ref[rows, :] = pick(group, [roll(four[0], 64), roll(four[1], 96), four[2], roll(four[3], 32)])
        second_ref[rows, :] = pick(group, [roll(four[0], 32), roll(four[1], 64), roll(four[2], 96), four[3]])


def score_call(tau, q_cols, keys, start, count):
    width = keys.shape[1]
    base = start // KEY_BLOCK
    steps = count // KEY_BLOCK
    half, quarter = KEY_BLOCK // 2, KEY_BLOCK // 4
    return pl.pallas_call(
        score_kernel,
        grid=(steps,),
        out_shape=(
            jax.ShapeDtypeStruct((count // 2, 128), F32),
            jax.ShapeDtypeStruct((count // 4, 128), F32),
            jax.ShapeDtypeStruct((count // 4, 128), F32),
        ),
        in_specs=[
            pl.BlockSpec(memory_space=SMEM),
            pl.BlockSpec((width, 128), lambda i: (0, 0)),
            pl.BlockSpec((KEY_BLOCK, width), lambda i: (i + base, 0)),
        ],
        out_specs=(
            pl.BlockSpec((half, 128), lambda i: (i, 0)),
            pl.BlockSpec((quarter, 128), lambda i: (i, 0)),
            pl.BlockSpec((quarter, 128), lambda i: (i, 0)),
        ),
        compiler_params=pltpu.CompilerParams(vmem_limit_bytes=24 * 2**20),
        cost_estimate=pl.CostEstimate(flops=2 * count * width * 128, bytes_accessed=2 * count * width, transcendentals=0),
        name="scores",
    )(tau, q_cols, keys)


def histogram_kernel(hists, n_parts, n_prev, line_ref, flag_ref, pos_ref, group_ref, *refs):
    parts, refs = refs[:n_parts], refs[n_parts:]
    prevs, refs = refs[:n_prev], refs[n_prev:]
    outs, refs = refs[: 4 * hists], refs[4 * hists :]
    scores, weights, hist, heads, in_sem, prev_sem, out_sem, head_sem = refs
    rows = scores.shape[0]
    lines = hist.shape[1]
    piece = lines // 4
    width = 128 // PACK * hists
    group = lane_group(128 // PACK)
    x, core = pos_ref[0], pos_ref[1]

    def piece_at(k):
        x_of = x if k >= 2 else 1 - x
        core_of = core if k % 2 else 1 - core
        return pl.ds(pl.multiple_of((2 * x_of + core_of) * piece, 8), piece)

    copies = []
    start = 0
    for i, part in enumerate(parts):
        copies.append(pltpu.make_async_copy(part, scores.at[pl.ds(start, part.shape[0])], in_sem.at[i]))
        copies[-1].start()
        start += part.shape[0]
    fetches = []
    for k in range(n_prev):
        fetches.append(pltpu.make_async_copy(prevs[k].at[pl.ds(0, piece)], hist.at[0, piece_at(k)], prev_sem.at[k]))
    if n_prev:
        fetches.append(pltpu.make_async_copy(prevs[0].at[pl.ds(piece, HEAD)], heads.at[1], prev_sem.at[n_prev]))
    for fetch in fetches:
        fetch.start()

    if not n_prev:
        clear_rows = 512

        def clear(i, carry):
            at = pl.ds(pl.multiple_of(i * clear_rows, clear_rows), clear_rows)
            hist[:, at, :] = jnp.zeros((hists, clear_rows, 128), F32)
            return carry

        lax.fori_loop(0, lines // clear_rows, clear, 0)
    for copy in copies:
        copy.wait()

    chunk = 256

    def top_of(i, best):
        block = scores[pl.ds(pl.multiple_of(i * chunk, chunk), chunk), :]
        return jnp.maximum(best, jnp.max(block.reshape(chunk // 8, 8, 128), axis=0))

    best = lax.fori_loop(0, rows // chunk, top_of, jnp.full((8, 128), -jnp.inf, F32))
    top = jnp.max(best, axis=0, keepdims=True)
    span = width
    while span < 128:
        top = jnp.maximum(top, roll(top, span))
        span *= 2

    if n_prev:
        for fetch in fetches:
            fetch.wait()
        old_top, old_total = heads[1, 0:1, :], heads[1, 1:2, :]
        top = jnp.maximum(top, old_top)
        old_scale = jnp.exp(old_top - top)
        scale_rows = 512

        def rescale(i, carry):
            at = pl.ds(pl.multiple_of(i * scale_rows, scale_rows), scale_rows)
            hist[0, at, :] = hist[0, at, :] * old_scale
            return carry

        lax.fori_loop(0, lines // scale_rows, rescale, 0)

    spread_lane = lax.broadcasted_iota(jnp.int32, (128, 128), 1) // width
    spread_row = lax.broadcasted_iota(jnp.int32, (128, 128), 0)
    keys_per_row = PACK // hists
    together = 2

    def spread(i, total):
        for u in range(together):
            block = i * together + u
            select = (spread_row == block * keys_per_row + spread_lane).astype(F32).astype(jnp.bfloat16)
            target = jnp.dot(group_ref[...], select, preferred_element_type=F32).astype(jnp.int32)
            shift = (target - group) & (PACK - 1)
            value = jnp.exp(scores[pl.ds(pl.multiple_of(block * 128, 128), 128), :] - top)
            total = total + jnp.sum(value.reshape(16, 8, 128), axis=0)
            turned = [jnp.where(shift == d, value, 0.0) for d in range(PACK)]
            turned = [turned[0]] + [roll(turned[d], 32 * d) for d in range(1, PACK)]
            for source in range(PACK):
                line = pick(group, [turned[(g - source) % PACK] for g in range(PACK)])
                at = pl.multiple_of((block * keys_per_row + source // hists) * 128, 128)
                weights[source % hists, pl.ds(at, 128), :] = line
        return total

    total = lax.fori_loop(0, rows // 128 // together, spread, jnp.zeros((8, 128), F32))
    total = jnp.sum(total, axis=0, keepdims=True)
    span = width
    while span < 128:
        total = total + roll(total, span)
        span *= 2

    def add(key, count):
        at = [line_ref[key + k] for k in range(count)]
        sums = [
            hist[h, pl.ds(at[k], 1), :] + weights[h, pl.ds(key + k, 1), :] for k in range(count) for h in range(hists)
        ]
        for k in range(count):
            for h in range(hists):
                hist[h, pl.ds(at[k], 1), :] = sums[k * hists + h]

    def add_keys(i, carry):
        key = i * FLAG_KEYS

        def apart():
            for b in range(FLAG_KEYS // BATCH_KEYS):
                add(key + b * BATCH_KEYS, BATCH_KEYS)

        def one_by_one():
            def step(k, carry):
                add(key + k, 1)
                return carry

            lax.fori_loop(0, FLAG_KEYS, step, 0)

        lax.cond(flag_ref[i] == 0, apart, one_by_one)
        return carry

    lax.fori_loop(0, weights.shape[1] // FLAG_KEYS, add_keys, 0)

    row = lax.broadcasted_iota(jnp.int32, (HEAD, 128), 0)
    if n_prev:
        tops, totals = [top], [total + old_total * old_scale]
    else:
        even = (group % 2) == 0
        tops, totals = [[jnp.where(even, v, roll(v, 32)), jnp.where(even, roll(v, 32), v)] for v in (top, total)]
    sends = []
    for h in range(hists):
        heads[h] = jnp.where(row == 0, tops[h], jnp.where(row == 1, totals[h], 0.0))
        for k in range(4):
            out = outs[k * hists + h]
            sends.append(pltpu.make_async_copy(hist.at[h, piece_at(k)], out.at[pl.ds(0, piece)], out_sem.at[h, k]))
            sends.append(pltpu.make_async_copy(heads.at[h], out.at[pl.ds(piece, HEAD)], head_sem.at[h, k]))
    for send in sends:
        send.start()
    for send in sends:
        send.wait()


def histogram_call(line, flags, pos, group, parts, prevs, vocab):
    hists = 1 if prevs else 2
    rows = sum(part.shape[0] for part in parts)
    lines = vocab // PACK
    out = jax.ShapeDtypeStruct((lines // 4 + HEAD, 128), F32)
    return pl.pallas_call(
        functools.partial(histogram_kernel, hists, len(parts), len(prevs)),
        out_shape=(out,) * (4 * hists),
        in_specs=[pl.BlockSpec(memory_space=SMEM)] * 3
        + [pl.BlockSpec(memory_space=VMEM)]
        + [pl.BlockSpec(memory_space=ANY)] * (len(parts) + len(prevs)),
        out_specs=(pl.BlockSpec(memory_space=ANY),) * (4 * hists),
        scratch_shapes=[
            VMEM((rows, 128), F32),
            VMEM((hists, line.shape[0], 128), F32),
            VMEM((hists, lines, 128), F32),
            VMEM((2, HEAD, 128), F32),
            pltpu.SemaphoreType.DMA((len(parts),)),
            pltpu.SemaphoreType.DMA((5,)),
            pltpu.SemaphoreType.DMA((hists, 4)),
            pltpu.SemaphoreType.DMA((hists, 4)),
        ],
        compiler_params=pltpu.CompilerParams(vmem_limit_bytes=(20 + 18 * hists) * 2**20),
        cost_estimate=pl.CostEstimate(flops=4 * 10**9, bytes_accessed=2 * 10**7, transcendentals=0),
        name="histogram",
    )(line, flags, pos, group, *parts, *prevs)


def place_ids(tok, vocab):
    piece = vocab // 4
    block = PACK * TOK_BLOCK
    part, within = tok // piece, tok % piece
    line = part * (piece // PACK) + (within // block) * TOK_BLOCK + within % TOK_BLOCK
    group = (within % block) // TOK_BLOCK
    batch = line.reshape(-1, BATCH_KEYS)
    meet = jnp.zeros(batch.shape[0], jnp.bool_)
    for shift in range(1, BATCH_KEYS):
        meet = meet | jnp.any(batch[:, shift:] == batch[:, :-shift], axis=1)
    flags = jnp.any(meet.reshape(-1, FLAG_KEYS // BATCH_KEYS), axis=1).astype(jnp.int32)
    return line, flags, group.reshape(-1, 128).T.astype(jnp.bfloat16)


def merge_kernel(a_ref, b_ref, out_ref):
    lines = a_ref.shape[0] - HEAD
    a_top, b_top = a_ref[lines : lines + 1, :], b_ref[lines : lines + 1, :]
    top = jnp.maximum(a_top, b_top)
    a_scale, b_scale = jnp.exp(a_top - top), jnp.exp(b_top - top)
    total = a_ref[lines + 1 : lines + 2, :] * a_scale + b_ref[lines + 1 : lines + 2, :] * b_scale
    chunk = 128

    def add(i, carry):
        at = pl.ds(pl.multiple_of(i * chunk, chunk), chunk)
        out_ref[at, :] = a_ref[at, :] * a_scale + b_ref[at, :] * b_scale
        return carry

    lax.fori_loop(0, lines // chunk, add, 0)
    row = lax.broadcasted_iota(jnp.int32, (HEAD, 128), 0)
    out_ref[lines : lines + HEAD, :] = jnp.where(row == 0, top, jnp.where(row == 1, total, 0.0))


def merge_call(a, b):
    return pl.pallas_call(
        merge_kernel,
        out_shape=jax.ShapeDtypeStruct(a.shape, F32),
        compiler_params=pltpu.CompilerParams(vmem_limit_bytes=16 * 2**20),
        cost_estimate=pl.CostEstimate(flops=10**8, bytes_accessed=3 * a.size * 4, transcendentals=0),
        name="merge",
    )(a, b)


def head_kernel(q_ref, w_ref, after_ref, logits_ref, stat_ref, top_ref, sum_ref):
    del after_ref
    i = pl.program_id(0)

    @pl.when(i == 0)
    def _():
        top_ref[...] = jnp.full(top_ref.shape, -jnp.inf, F32)
        sum_ref[...] = jnp.zeros(sum_ref.shape, F32)

    logits = jnp.dot(q_ref[...], w_ref[...], preferred_element_type=F32)
    logits_ref[...] = logits
    old = top_ref[...]
    new = jnp.maximum(old, jnp.max(logits, axis=1, keepdims=True))
    part = jnp.sum(jnp.exp(logits - new[:, 0:1]), axis=1, keepdims=True)
    sum_ref[...] = sum_ref[...] * jnp.exp(old - new) + part
    top_ref[...] = new
    stat_ref[0] = top_ref[...]
    stat_ref[1] = sum_ref[...]


def head_call(rows, w_head, after):
    count, width = rows.shape
    cols = w_head.shape[1]
    block = cols // 10
    return pl.pallas_call(
        head_kernel,
        grid=(cols // block,),
        out_shape=(jax.ShapeDtypeStruct((count, cols), F32), jax.ShapeDtypeStruct((2, count, 128), F32)),
        in_specs=[
            pl.BlockSpec((count, width), lambda i: (0, 0)),
            pl.BlockSpec((width, block), lambda i: (0, i)),
            pl.BlockSpec(memory_space=ANY),
        ],
        out_specs=(pl.BlockSpec((count, block), lambda i: (0, i)), pl.BlockSpec((2, count, 128), lambda i: (0, 0, 0))),
        scratch_shapes=[VMEM((count, 128), F32), VMEM((count, 128), F32)],
        compiler_params=pltpu.CompilerParams(vmem_limit_bytes=24 * 2**20),
        cost_estimate=pl.CostEstimate(flops=2 * count * width * cols, bytes_accessed=2 * width * cols, transcendentals=0),
        name="head",
    )(rows, w_head, after)


def mix_kernel(n_prev, mix_ref, *refs):
    ins, heads, logits_ref, stat_ref = refs[:3], refs[3:6], refs[6], refs[7]
    out_ref = refs[8 + n_prev]
    mix = mix_ref[0]
    tops = [head[0:1, :] for head in heads]
    top = jnp.maximum(jnp.maximum(tops[0], tops[1]), tops[2])
    scales = [jnp.exp(value - top) for value in tops]
    total = sum(head[1:2, :] * scale for head, scale in zip(heads, scales))
    scales = [scale * mix / total for scale in scales]
    lm_top = stat_ref[0]
    lm_scale = (1.0 - mix) / stat_ref[1]
    for b in range(STAGE_BLOCKS):
        rows = slice(b * TOK_BLOCK, (b + 1) * TOK_BLOCK)
        value = ins[0][rows, :] * scales[0] + ins[1][rows, :] * scales[1] + ins[2][rows, :] * scales[2]
        turned = value.T
        for g in range(PACK):
            cols = slice((b * PACK + g) * TOK_BLOCK, (b * PACK + g + 1) * TOK_BLOCK)
            lm = jnp.exp(logits_ref[:, cols] - lm_top) * lm_scale
            out_ref[:, cols] = jnp.log(turned[g * 32 : (g + 1) * 32, :] + lm)


def mix_call(mix, pieces, logits, stat, index, prev):
    lines = pieces[0].shape[0] - HEAD
    block = STAGE_BLOCKS * TOK_BLOCK
    count, cols = logits.shape
    n_prev = 0 if prev is None else 1
    wide = block * PACK
    return pl.pallas_call(
        functools.partial(mix_kernel, n_prev),
        grid=(lines // block,),
        out_shape=jax.ShapeDtypeStruct((count, cols), F32),
        in_specs=[pl.BlockSpec(memory_space=SMEM)]
        + [pl.BlockSpec((block, 128), lambda i: (i, 0))] * 3
        + [pl.BlockSpec((HEAD, 128), lambda i: (lines // HEAD, 0))] * 3
        + [pl.BlockSpec((32, wide), lambda i: (index, i)), pl.BlockSpec((2, 32, 128), lambda i: (0, index, 0))]
        + [pl.BlockSpec(memory_space=ANY)] * n_prev,
        out_specs=pl.BlockSpec((32, wide), lambda i: (index, i)),
        input_output_aliases={9: 0} if n_prev else {},
        compiler_params=pltpu.CompilerParams(vmem_limit_bytes=16 * 2**20),
        cost_estimate=pl.CostEstimate(flops=10**8, bytes_accessed=8 * 10**6, transcendentals=0),
        name="mix",
    )(mix, *pieces, *pieces, logits, stat, *([prev] if n_prev else []))


CHUNKS = (2048, 4096, 4096, 6144)


def solution(mesh):
    store_devs = mesh.shape["store"]
    model_devs = mesh.shape["model"]
    assert store_devs == 2 and model_devs == 4
    group_axes = ("store", "model")
    across_y = [(0, 1), (1, 0)]
    across_core = [(0, 1), (1, 0), (2, 3), (3, 2)]
    across_x = [(0, 2), (2, 0), (1, 3), (3, 1)]

    def swap_y(value):
        return lax.ppermute(value, "store", across_y)

    def swap_core(value):
        return lax.ppermute(value, "model", across_core)

    def swap_x(value):
        return lax.ppermute(value, "model", across_x)

    def local_step(queries, w_head, store_keys, store_tok, temperature, mix_weight):
        vocab = w_head.shape[1] * model_devs
        rows = queries.shape[0] // store_devs
        y = lax.axis_index("store")
        m = lax.axis_index("model")
        pos = jnp.stack([m // 2, m % 2]).astype(jnp.int32)
        mine = lax.dynamic_slice_in_dim(queries, y * rows, rows, axis=0)
        theirs = lax.dynamic_slice_in_dim(queries, (1 - y) * rows, rows, axis=0)
        q_cols = jnp.concatenate([mine, theirs], axis=0).T
        tau = temperature.reshape(1)
        mix = mix_weight.reshape(1)

        their_tok = swap_y(store_tok)
        own, first, second = [], [], []
        start = 0
        for count in CHUNKS:
            a, b, c = score_call(tau, q_cols, store_keys, start, count)
            own.append(a)
            first.append(swap_y(b))
            second.append(c)
            start += count
        second = [swap_y(part) for part in second]

        own_line, own_flags, own_group = place_ids(store_tok, vocab)
        line, flags, group = place_ids(their_tok, vocab)
        kept = histogram_call(own_line, own_flags, pos, own_group, own, [], vocab)
        sums = []
        for index, parts in enumerate((first, second)):
            out = histogram_call(line, flags, pos, group, parts, kept[index::2], vocab)
            far = swap_x(merge_call(out[1], swap_core(out[0])))
            sums.append((out[3], swap_core(out[2]), far))
            last = out[3]
        logits, stat = head_call(mine, w_head, last)
        for swap in (swap_core, swap_x):
            other = swap(stat)
            top = jnp.maximum(stat[0], other[0])
            stat = jnp.stack([top, stat[1] * jnp.exp(stat[0] - top) + other[1] * jnp.exp(other[0] - top)])
        result = mix_call(mix, sums[0], logits, stat, 0, None)
        return mix_call(mix, sums[1], logits, stat, 1, result)

    return jax.shard_map(
        local_step,
        mesh=mesh,
        in_specs=(P("data", None), P(None, "model"), P(group_axes, None), P(group_axes), P(), P()),
        out_specs=P(("data", "store"), "model"),
        check_vma=False,
    )
```

```python
import functools

import jax
import jax.numpy as jnp
from jax import lax
from jax.experimental import pallas as pl
from jax.experimental.pallas import tpu as pltpu
from jax.sharding import PartitionSpec as P


F32 = jnp.float32
ANY = pl.ANY
VMEM = pltpu.VMEM
SMEM = pltpu.SMEM
KEY_BLOCK = 1024
VMEM_BYTES = 63 * 2**20
BATCH_KEYS = 8
FLAG_KEYS = 128
PACK = 4
TOK_BLOCK = 128
ORDERS = ((0, 2, 1, 3), (3, 0, 2, 1))
STAGE_BLOCKS = 5
HEAD = 8


def lane_group(width):
    return lax.broadcasted_iota(jnp.int32, (1, 128), 1) // width


def pick(group, parts):
    out = parts[-1]
    for index in range(len(parts) - 2, -1, -1):
        out = jnp.where(group == index, parts[index], out)
    return out


def roll(value, shift):
    return pltpu.roll(value, shift % 128, 1)


def score_kernel(tau_ref, q_ref, k_ref, own_ref, first_ref, second_ref):
    tau = tau_ref[0]
    dots = jnp.dot(k_ref[...], q_ref[...], preferred_element_type=F32)
    step = 128
    norms = []
    for row in range(0, KEY_BLOCK, step):
        acc = jnp.zeros((step, 128), F32)
        for col in range(0, k_ref.shape[1], 128):
            part = k_ref[row : row + step, col : col + 128].astype(F32)
            acc += part * part
        norms.append(jnp.sum(acc, axis=1, keepdims=True))
    group = lane_group(32)
    scores = [(2.0 * dots[i * step : (i + 1) * step] - norms[i]) / tau for i in range(KEY_BLOCK // step)]
    for i in range(KEY_BLOCK // step // 2):
        own_ref[i * step : (i + 1) * step, :] = jnp.where(group < 2, scores[2 * i], roll(scores[2 * i + 1], 64))
    for i in range(KEY_BLOCK // step // 4):
        four = scores[4 * i : 4 * i + 4]
        rows = slice(i * step, (i + 1) * step)
        first_ref[rows, :] = pick(group, [roll(four[0], 64), roll(four[1], 96), four[2], roll(four[3], 32)])
        second_ref[rows, :] = pick(group, [roll(four[0], 32), roll(four[1], 64), roll(four[2], 96), four[3]])


def score_call(tau, q_cols, keys, start, count):
    width = keys.shape[1]
    base = start // KEY_BLOCK
    steps = count // KEY_BLOCK
    half, quarter = KEY_BLOCK // 2, KEY_BLOCK // 4
    return pl.pallas_call(
        score_kernel,
        grid=(steps,),
        out_shape=(
            jax.ShapeDtypeStruct((count // 2, 128), F32),
            jax.ShapeDtypeStruct((count // 4, 128), F32),
            jax.ShapeDtypeStruct((count // 4, 128), F32),
        ),
        in_specs=[
            pl.BlockSpec(memory_space=SMEM),
            pl.BlockSpec((width, 128), lambda i: (0, 0)),
            pl.BlockSpec((KEY_BLOCK, width), lambda i: (i + base, 0)),
        ],
        out_specs=(
            pl.BlockSpec((half, 128), lambda i: (i, 0)),
            pl.BlockSpec((quarter, 128), lambda i: (i, 0)),
            pl.BlockSpec((quarter, 128), lambda i: (i, 0)),
        ),
        compiler_params=pltpu.CompilerParams(vmem_limit_bytes=VMEM_BYTES),
        cost_estimate=pl.CostEstimate(flops=2 * count * width * 128, bytes_accessed=2 * count * width, transcendentals=0),
        name="scores",
    )(tau, q_cols, keys)


def place_ids(tok_ref, order, group_ref, ids_ref, line_ref, flag_ref, sem):
    assert PACK == 4 and TOK_BLOCK == 128
    tok = tok_ref[...]
    block, run, within = tok >> 9, (tok >> 7) & 3, tok & 127
    if order is None:
        line = block * 256 + (run >> 1) * 128 + within
        group = run & 1
    else:
        line = block * 128 + within
        group = sum(jnp.where(run == order[g], g, 0) for g in range(PACK))
    lane = lax.broadcasted_iota(jnp.int32, (1, 128), 1)
    meet = jnp.zeros(tok.shape, F32)
    for shift in range(1, BATCH_KEYS):
        same = (line == roll(line, shift)) & (lane % BATCH_KEYS >= shift)
        meet = jnp.where(same, 1.0, meet)
    rows = lax.broadcasted_iota(jnp.int32, (128, 128), 0) // FLAG_KEYS
    shared = (rows == lax.broadcasted_iota(jnp.int32, (128, 128), 1) // FLAG_KEYS).astype(F32)
    ids_ref[0] = line
    ids_ref[1] = jnp.dot(meet, shared, preferred_element_type=F32).astype(jnp.int32)
    group_ref[...] = group.astype(F32).T.astype(jnp.bfloat16)
    return [
        pltpu.make_async_copy(ids_ref.at[0], line_ref, sem.at[0]),
        pltpu.make_async_copy(ids_ref.at[1], flag_ref, sem.at[1]),
    ]


def load_parts(parts, scores, sem):
    copies = []
    start = 0
    for i, part in enumerate(parts):
        copies.append(pltpu.make_async_copy(part, scores.at[pl.ds(start, part.shape[0])], sem.at[i]))
        copies[-1].start()
        start += part.shape[0]
    return copies


def clear(hist):
    step = 512

    def body(i, carry):
        hist[pl.ds(pl.multiple_of(i * step, step), step), :] = jnp.zeros((step, 128), F32)
        return carry

    lax.fori_loop(0, hist.shape[0] // step, body, 0)


def across(value, width, combine):
    while width < 128:
        value = combine(value, roll(value, width))
        width *= 2
    return value


def top_of(scores, width):
    step = 512

    def body(i, best):
        block = scores[pl.ds(pl.multiple_of(i * step, step), step), :]
        return jnp.maximum(best, jnp.max(block.reshape(step // 8, 8, 128), axis=0))

    best = lax.fori_loop(0, scores.shape[0] // step, body, jnp.full((8, 128), -jnp.inf, F32))
    return across(jnp.max(best, axis=0, keepdims=True), width, jnp.maximum)


def spread_weights(scores, weights, group_ref, top, width):
    count = 128 // width
    group = lane_group(width)
    spread_lane = lax.broadcasted_iota(jnp.int32, (128, 128), 1) // width
    spread_row = lax.broadcasted_iota(jnp.int32, (128, 128), 0)
    together = 4

    def body(i, total):
        for u in range(together):
            block = i * together + u
            select = (spread_row == block * count + spread_lane).astype(F32).astype(jnp.bfloat16)
            target = jnp.dot(group_ref[...], select, preferred_element_type=F32).astype(jnp.int32)
            shift = (target - group) & (count - 1)
            value = jnp.exp(scores[pl.ds(pl.multiple_of(block * 128, 128), 128), :] - top)
            total = total + jnp.sum(value.reshape(16, 8, 128), axis=0)
            turned = [jnp.where(shift == d, value, 0.0) for d in range(count)]
            turned = [turned[0]] + [roll(turned[d], width * d) for d in range(1, count)]
            for source in range(count):
                line = pick(group, [turned[(g - source) % count] for g in range(count)])
                at = pl.multiple_of((block * count + source) * 128, 128)
                weights[pl.ds(at, 128), :] = line
        return total

    total = lax.fori_loop(0, scores.shape[0] // 128 // together, body, jnp.zeros((8, 128), F32))
    return across(jnp.sum(total, axis=0, keepdims=True), width, jnp.add)


def add_weights(line_ref, flag_ref, weights, hists):
    assert FLAG_KEYS == 128

    def add(hist, row, lane, key, count):
        at = [line_ref[row, lane + k] for k in range(count)]
        sums = [hist[pl.ds(at[k], 1), :] + weights[pl.ds(key + k, 1), :] for k in range(count)]
        for k in range(count):
            hist[pl.ds(at[k], 1), :] = sums[k]

    def body(i, carry):
        key = i * FLAG_KEYS

        def apart():
            for b in range(FLAG_KEYS // BATCH_KEYS):
                add(hists[b % 2], i, b * BATCH_KEYS, key + b * BATCH_KEYS, BATCH_KEYS)

        def one_by_one():
            def step(k, carry):
                for which in range(2):
                    add(hists[which], i, 2 * k + which, key + 2 * k + which, 1)
                return carry

            lax.fori_loop(0, FLAG_KEYS // 2, step, 0)

        lax.cond(flag_ref[i, 0] == 0, apart, one_by_one)
        return carry

    lax.fori_loop(0, weights.shape[0] // FLAG_KEYS, body, 0)


def piece_at(pos_ref, k, size):
    x, core = pos_ref[0], pos_ref[1]
    x_of = x if k >= 2 else 1 - x
    core_of = core if k % 2 else 1 - core
    return pl.ds(pl.multiple_of((2 * x_of + core_of) * size, 8), size)


def head_block(top, total):
    row = lax.broadcasted_iota(jnp.int32, (HEAD, 128), 0)
    return jnp.where(row == 0, top, jnp.where(row == 1, total, 0.0))


def own_kernel(order, n_parts, pos_ref, tok_ref, *refs):
    parts, refs = refs[:n_parts], refs[n_parts:]
    outs, refs = refs[:8], refs[8:]
    group_ref, ids_ref, line_ref, flag_ref, id_sem, scores, weights, even, odd, heads, in_sem, out_sem, head_sem = refs
    lines = even.shape[0]
    piece = lines // 8
    copies = load_parts(parts, scores, in_sem)
    copies += place_ids(tok_ref, order, group_ref, ids_ref, line_ref, flag_ref, id_sem)
    for copy in copies[-2:]:
        copy.start()
    clear(even)
    clear(odd)
    for copy in copies:
        copy.wait()
    top = top_of(scores, 64)
    total = spread_weights(scores, weights, group_ref, top, 64)
    add_weights(line_ref, flag_ref, weights, (even, odd))

    quad = lane_group(32) % 2 == 0
    tops = [jnp.where(quad, top, roll(top, 32)), jnp.where(quad, roll(top, 32), top)]
    totals = [jnp.where(quad, total, roll(total, 32)), jnp.where(quad, roll(total, 32), total)]
    for c in range(2):
        heads[c] = head_block(tops[c], totals[c])
    together = 4

    def split(i, carry):
        values = []
        for u in range(together):
            block = i * together + u
            near = pl.ds(pl.multiple_of(block * 256, 256), 128)
            far = pl.ds(pl.multiple_of(block * 256 + 128, 128), 128)
            low = even[near, :] + odd[near, :]
            high = roll(even[far, :] + odd[far, :], 32)
            values.append((block, low, high))
        for block, low, high in values:
            at = pl.ds(pl.multiple_of(block * 128, 128), 128)
            weights[at, :] = jnp.where(quad, low, high)
            even[at, :] = jnp.where(quad, high, low)
        return carry

    lax.fori_loop(0, lines // 256 // together, split, 0)
    sends = []
    for c, source in enumerate((weights, even)):
        for k in range(4):
            out = outs[k * 2 + c]
            at = piece_at(pos_ref, k, piece)
            sends.append(pltpu.make_async_copy(source.at[at], out.at[pl.ds(0, piece)], out_sem.at[c, k]))
            sends.append(pltpu.make_async_copy(heads.at[c], out.at[pl.ds(piece, HEAD)], head_sem.at[c, k]))
    for send in sends:
        send.start()
    for send in sends:
        send.wait()


def chunk_kernel(order, n_parts, pos_ref, tok_ref, *refs):
    parts, refs = refs[:n_parts], refs[n_parts:]
    prevs, refs = refs[:4], refs[5:]
    outs, refs = refs[:4], refs[4:]
    group_ref, ids_ref, line_ref, flag_ref, id_sem, scores, weights, even, odd, heads, in_sem, prev_sem, out_sem, head_sem = refs
    lines = even.shape[0]
    piece = lines // 4
    copies = load_parts(parts, scores, in_sem)
    fetches = [
        pltpu.make_async_copy(prevs[k].at[pl.ds(0, piece)], even.at[piece_at(pos_ref, k, piece)], prev_sem.at[k])
        for k in range(4)
    ]
    fetches.append(pltpu.make_async_copy(prevs[0].at[pl.ds(piece, HEAD)], heads.at[1], prev_sem.at[4]))
    for fetch in fetches:
        fetch.start()
    copies += place_ids(tok_ref, order, group_ref, ids_ref, line_ref, flag_ref, id_sem)
    for copy in copies[-2:]:
        copy.start()
    clear(odd)
    for copy in copies:
        copy.wait()
    top = top_of(scores, 32)
    for fetch in fetches:
        fetch.wait()
    old_top, old_total = heads[1, 0:1, :], heads[1, 1:2, :]
    top = jnp.maximum(top, old_top)
    old_scale = jnp.exp(old_top - top)
    total = spread_weights(scores, weights, group_ref, top, 32)
    step = 256

    def rescale(i, carry):
        at = pl.ds(pl.multiple_of(i * step, step), step)
        even[at, :] = even[at, :] * old_scale
        return carry

    lax.fori_loop(0, lines // step, rescale, 0)
    add_weights(line_ref, flag_ref, weights, (even, odd))

    def join(i, carry):
        at = pl.ds(pl.multiple_of(i * step, step), step)
        even[at, :] = even[at, :] + odd[at, :]
        return carry

    lax.fori_loop(0, lines // step, join, 0)
    heads[0] = head_block(top, total + old_total * old_scale)
    sends = []
    for k in range(4):
        at = piece_at(pos_ref, k, piece)
        sends.append(pltpu.make_async_copy(even.at[at], outs[k].at[pl.ds(0, piece)], out_sem.at[k]))
        sends.append(pltpu.make_async_copy(heads.at[0], outs[k].at[pl.ds(piece, HEAD)], head_sem.at[k]))
    for send in sends:
        send.start()
    for send in sends:
        send.wait()


def histogram_call(tok, order, pos, parts, prevs, after, vocab):
    own = not prevs
    rows = sum(part.shape[0] for part in parts)
    lines = vocab // (2 if own else PACK)
    out = jax.ShapeDtypeStruct((vocab // PACK // 4 + HEAD, 128), F32)
    keys = tok.shape[0]
    tok = tok.reshape(128, 128)
    assert keys == 128 * 128
    count = 8 if own else 4
    dma = pltpu.SemaphoreType.DMA
    extra = [] if own else [*prevs, after]
    return pl.pallas_call(
        functools.partial(own_kernel if own else chunk_kernel, order, len(parts)),
        out_shape=(out,) * count,
        in_specs=[pl.BlockSpec(memory_space=SMEM), pl.BlockSpec(memory_space=VMEM)]
        + [pl.BlockSpec(memory_space=ANY)] * (len(parts) + len(extra)),
        out_specs=(pl.BlockSpec(memory_space=ANY),) * count,
        scratch_shapes=[VMEM((128, 128), jnp.bfloat16), VMEM((2, 128, 128), jnp.int32)]
        + [SMEM((128, 128), jnp.int32), SMEM((128, 128), jnp.int32), dma((2,))]
        + [VMEM((rows, 128), F32), VMEM((keys, 128), F32), VMEM((lines, 128), F32), VMEM((lines, 128), F32)]
        + [VMEM((2, HEAD, 128), F32), dma((len(parts),))]
        + ([dma((2, 4)), dma((2, 4))] if own else [dma((5,)), dma((4,)), dma((4,))]),
        compiler_params=pltpu.CompilerParams(vmem_limit_bytes=VMEM_BYTES),
        cost_estimate=pl.CostEstimate(flops=10**6, bytes_accessed=2 * 10**7, transcendentals=0),
        name="own_histogram" if own else "chunk_histogram",
    )(pos, tok, *parts, *extra)


def merge_kernel(a_ref, b_ref, out_ref):
    lines = a_ref.shape[0] - HEAD
    a_top, b_top = a_ref[lines : lines + 1, :], b_ref[lines : lines + 1, :]
    top = jnp.maximum(a_top, b_top)
    a_scale, b_scale = jnp.exp(a_top - top), jnp.exp(b_top - top)
    total = a_ref[lines + 1 : lines + 2, :] * a_scale + b_ref[lines + 1 : lines + 2, :] * b_scale
    chunk = 128

    def add(i, carry):
        at = pl.ds(pl.multiple_of(i * chunk, chunk), chunk)
        out_ref[at, :] = a_ref[at, :] * a_scale + b_ref[at, :] * b_scale
        return carry

    lax.fori_loop(0, lines // chunk, add, 0)
    row = lax.broadcasted_iota(jnp.int32, (HEAD, 128), 0)
    out_ref[lines : lines + HEAD, :] = jnp.where(row == 0, top, jnp.where(row == 1, total, 0.0))


def merge_call(a, b):
    return pl.pallas_call(
        merge_kernel,
        out_shape=jax.ShapeDtypeStruct(a.shape, F32),
        compiler_params=pltpu.CompilerParams(vmem_limit_bytes=VMEM_BYTES),
        cost_estimate=pl.CostEstimate(flops=10**5, bytes_accessed=3 * a.size * 4, transcendentals=0),
        name="merge",
    )(a, b)


def head_kernel(q_ref, w_ref, after_ref, logits_ref, stat_ref, top_ref, sum_ref):
    del after_ref
    i = pl.program_id(0)

    @pl.when(i == 0)
    def _():
        top_ref[...] = jnp.full(top_ref.shape, -jnp.inf, F32)
        sum_ref[...] = jnp.zeros(sum_ref.shape, F32)

    logits = jnp.dot(q_ref[...], w_ref[...], preferred_element_type=F32)
    logits_ref[...] = logits
    old = top_ref[...]
    new = jnp.maximum(old, jnp.max(logits, axis=1, keepdims=True))
    part = jnp.sum(jnp.exp(logits - new[:, 0:1]), axis=1, keepdims=True)
    sum_ref[...] = sum_ref[...] * jnp.exp(old - new) + part
    top_ref[...] = new
    stat_ref[0] = top_ref[...]
    stat_ref[1] = sum_ref[...]


def head_call(rows, w_head, after):
    count, width = rows.shape
    cols = w_head.shape[1]
    block = cols // 10
    return pl.pallas_call(
        head_kernel,
        grid=(cols // block,),
        out_shape=(jax.ShapeDtypeStruct((count, cols), F32), jax.ShapeDtypeStruct((2, count, 128), F32)),
        in_specs=[
            pl.BlockSpec((count, width), lambda i: (0, 0)),
            pl.BlockSpec((width, block), lambda i: (0, i)),
            pl.BlockSpec(memory_space=ANY),
        ],
        out_specs=(pl.BlockSpec((count, block), lambda i: (0, i)), pl.BlockSpec((2, count, 128), lambda i: (0, 0, 0))),
        scratch_shapes=[VMEM((count, 128), F32), VMEM((count, 128), F32)],
        compiler_params=pltpu.CompilerParams(vmem_limit_bytes=VMEM_BYTES),
        cost_estimate=pl.CostEstimate(flops=2 * count * width * cols, bytes_accessed=2 * width * cols, transcendentals=0),
        name="head",
    )(rows, w_head, after)


def mix_kernel(order, n_prev, mix_ref, *refs):
    ins, heads, logits_ref, stat_ref = refs[:3], refs[3:6], refs[6], refs[7]
    out_ref = refs[8 + n_prev]
    mix = mix_ref[0]
    tops = [head[0:1, :] for head in heads]
    top = jnp.maximum(jnp.maximum(tops[0], tops[1]), tops[2])
    scales = [jnp.exp(value - top) for value in tops]
    total = sum(head[1:2, :] * scale for head, scale in zip(heads, scales))
    scales = [scale * mix / total for scale in scales]
    lm_top = stat_ref[0]
    lm_scale = (1.0 - mix) / stat_ref[1]
    for b in range(STAGE_BLOCKS):
        rows = slice(b * TOK_BLOCK, (b + 1) * TOK_BLOCK)
        value = ins[0][rows, :] * scales[0] + ins[1][rows, :] * scales[1] + ins[2][rows, :] * scales[2]
        turned = value.T
        for g in range(PACK):
            run = order[g]
            cols = slice((b * PACK + run) * TOK_BLOCK, (b * PACK + run + 1) * TOK_BLOCK)
            lm = jnp.exp(logits_ref[:, cols] - lm_top) * lm_scale
            out_ref[:, cols] = jnp.log(turned[g * 32 : (g + 1) * 32, :] + lm)


def mix_call(mix, pieces, logits, stat, index, prev):
    lines = pieces[0].shape[0] - HEAD
    block = STAGE_BLOCKS * TOK_BLOCK
    count, cols = logits.shape
    n_prev = 0 if prev is None else 1
    wide = block * PACK
    return pl.pallas_call(
        functools.partial(mix_kernel, ORDERS[index], n_prev),
        grid=(lines // block,),
        out_shape=jax.ShapeDtypeStruct((count, cols), F32),
        in_specs=[pl.BlockSpec(memory_space=SMEM)]
        + [pl.BlockSpec((block, 128), lambda i: (i, 0))] * 3
        + [pl.BlockSpec((HEAD, 128), lambda i: (lines // HEAD, 0))] * 3
        + [pl.BlockSpec((32, wide), lambda i: (index, i)), pl.BlockSpec((2, 32, 128), lambda i: (0, index, 0))]
        + [pl.BlockSpec(memory_space=ANY)] * n_prev,
        out_specs=pl.BlockSpec((32, wide), lambda i: (index, i)),
        input_output_aliases={9: 0} if n_prev else {},
        compiler_params=pltpu.CompilerParams(vmem_limit_bytes=VMEM_BYTES),
        cost_estimate=pl.CostEstimate(flops=10**5, bytes_accessed=8 * 10**6, transcendentals=0),
        name="mix",
    )(mix, *pieces, *pieces, logits, stat, *([prev] if n_prev else []))


CHUNKS = (2048, 6144, 8192)


def solution(mesh):
    store_devs = mesh.shape["store"]
    model_devs = mesh.shape["model"]
    assert store_devs == 2 and model_devs == 4
    group_axes = ("store", "model")
    across_y = [(0, 1), (1, 0)]
    across_core = [(0, 1), (1, 0), (2, 3), (3, 2)]
    across_x = [(0, 2), (2, 0), (1, 3), (3, 1)]

    def swap_y(value):
        return lax.ppermute(value, "store", across_y)

    def swap_core(value):
        return lax.ppermute(value, "model", across_core)

    def swap_x(value):
        return lax.ppermute(value, "model", across_x)

    def local_step(queries, w_head, store_keys, store_tok, temperature, mix_weight):
        vocab = w_head.shape[1] * model_devs
        rows = queries.shape[0] // store_devs
        y = lax.axis_index("store")
        m = lax.axis_index("model")
        pos = jnp.stack([m // 2, m % 2]).astype(jnp.int32)
        mine = lax.dynamic_slice_in_dim(queries, y * rows, rows, axis=0)
        theirs = lax.dynamic_slice_in_dim(queries, (1 - y) * rows, rows, axis=0)
        q_cols = jnp.concatenate([mine, theirs], axis=0).T
        tau = temperature.reshape(1)
        mix = mix_weight.reshape(1)

        their_tok = swap_y(store_tok)
        own, first, second = [], [], []
        start = 0
        for count in CHUNKS:
            a, b, c = score_call(tau, q_cols, store_keys, start, count)
            own.append(a)
            first.append(swap_y(b))
            second.append(swap_y(c))
            start += count

        kept = histogram_call(store_tok, None, pos, own, [], None, vocab)
        sums = []
        after = kept[0]
        for index, parts in enumerate((first, second)):
            out = histogram_call(their_tok, ORDERS[index], pos, parts, kept[index::2], after, vocab)
            far = swap_core(out[0])
            near = swap_core(out[2])
            after = merge_call(out[1], far)
            sums.append((out[3], near, swap_x(after)))
            last = out[3]
        logits, stat = head_call(mine, w_head, last)
        for swap in (swap_core, swap_x):
            other = swap(stat)
            top = jnp.maximum(stat[0], other[0])
            stat = jnp.stack([top, stat[1] * jnp.exp(stat[0] - top) + other[1] * jnp.exp(other[0] - top)])
        result = mix_call(mix, sums[0], logits, stat, 0, None)
        return mix_call(mix, sums[1], logits, stat, 1, result)

    return jax.shard_map(
        local_step,
        mesh=mesh,
        in_specs=(P("data", None), P(None, "model"), P(group_axes, None), P(group_axes), P(), P()),
        out_specs=P(("data", "store"), "model"),
        check_vma=False,
    )
```

```python
import functools

import jax
import jax.numpy as jnp
from jax import lax
from jax.experimental import pallas as pl
from jax.experimental.pallas import tpu as pltpu
from jax.sharding import PartitionSpec as P


F32 = jnp.float32
ANY = pl.ANY
VMEM = pltpu.VMEM
SMEM = pltpu.SMEM
KEY_BLOCK = 1024
VMEM_BYTES = 63 * 2**20
BATCH_KEYS = 8
FLAG_KEYS = 128
PACK = 4
TOK_BLOCK = 128
ORDERS = ((0, 2, 1, 3), (3, 0, 2, 1))
STAGE_BLOCKS = 5
HEAD = 8


def lane_group(width):
    return lax.broadcasted_iota(jnp.int32, (1, 128), 1) // width


def pick(group, parts):
    out = parts[-1]
    for index in range(len(parts) - 2, -1, -1):
        out = jnp.where(group == index, parts[index], out)
    return out


def roll(value, shift):
    return pltpu.roll(value, shift % 128, 1)


def score_kernel(tau_ref, rows_ref, k_ref, own_ref, *sent):
    *sent, q_ref = sent
    tau = tau_ref[0]
    first_ref, second_ref = (sent[0].at[0], sent[0].at[1]) if len(sent) == 1 else sent

    @pl.when(pl.program_id(0) == 0)
    def _():
        half = q_ref.shape[0] // 2
        y = lax.axis_index("store")
        q_ref[0:half, :] = rows_ref[pl.ds(pl.multiple_of(y * half, half), half), :]
        q_ref[half : 2 * half, :] = rows_ref[pl.ds(pl.multiple_of((1 - y) * half, half), half), :]

    dots = lax.dot_general(k_ref[...], q_ref[...], (((1,), (1,)), ((), ())), preferred_element_type=F32)
    step = 128
    norms = []
    for row in range(0, KEY_BLOCK, step):
        acc = jnp.zeros((step, 128), F32)
        for col in range(0, k_ref.shape[1], 128):
            part = k_ref[row : row + step, col : col + 128].astype(F32)
            acc += part * part
        norms.append(jnp.sum(acc, axis=1, keepdims=True))
    group = lane_group(32)
    scores = [(2.0 * dots[i * step : (i + 1) * step] - norms[i]) / tau for i in range(KEY_BLOCK // step)]
    for i in range(KEY_BLOCK // step // 2):
        own_ref[i * step : (i + 1) * step, :] = jnp.where(group < 2, scores[2 * i], roll(scores[2 * i + 1], 64))
    for i in range(KEY_BLOCK // step // 4):
        four = scores[4 * i : 4 * i + 4]
        rows = slice(i * step, (i + 1) * step)
        first_ref[rows, :] = pick(group, [roll(four[0], 64), roll(four[1], 96), four[2], roll(four[3], 32)])
        second_ref[rows, :] = pick(group, [roll(four[0], 32), roll(four[1], 64), roll(four[2], 96), four[3]])


def score_call(tau, queries, keys, start, count, joined):
    width = keys.shape[1]
    base = start // KEY_BLOCK
    half, quarter = KEY_BLOCK // 2, KEY_BLOCK // 4
    if joined:
        sent_shape = (jax.ShapeDtypeStruct((2, count // 4, 128), F32),)
        sent_spec = (pl.BlockSpec((2, quarter, 128), lambda i: (0, i, 0)),)
    else:
        sent_shape = (jax.ShapeDtypeStruct((count // 4, 128), F32),) * 2
        sent_spec = (pl.BlockSpec((quarter, 128), lambda i: (i, 0)),) * 2
    return pl.pallas_call(
        score_kernel,
        grid=(count // KEY_BLOCK,),
        out_shape=(jax.ShapeDtypeStruct((count // 2, 128), F32),) + sent_shape,
        in_specs=[
            pl.BlockSpec(memory_space=SMEM),
            pl.BlockSpec((128, width), lambda i: (0, 0)),
            pl.BlockSpec((KEY_BLOCK, width), lambda i: (i + base, 0)),
        ],
        out_specs=(pl.BlockSpec((half, 128), lambda i: (i, 0)),) + sent_spec,
        scratch_shapes=[VMEM((128, width), jnp.bfloat16)],
        compiler_params=pltpu.CompilerParams(vmem_limit_bytes=VMEM_BYTES),
        cost_estimate=pl.CostEstimate(flops=2 * count * width * 128, bytes_accessed=2 * count * width, transcendentals=0),
        name="scores",
    )(tau, queries, keys)


def place_ids(tok_ref, which, group_ref, ids_ref, line_ref, flag_ref, sem):
    assert PACK == 4 and TOK_BLOCK == 128
    tok = tok_ref[...]
    block, run, within = tok >> 9, (tok >> 7) & 3, tok & 127
    if which is None:
        line = block * 256 + (run >> 1) * 128 + within
        group = run & 1
    else:
        line = block * 128 + within
        group = sum(jnp.where(run == ORDERS[which][g], g, 0) for g in range(PACK))
    lane = lax.broadcasted_iota(jnp.int32, (1, 128), 1)
    meet = jnp.zeros(tok.shape, F32)
    for shift in range(1, BATCH_KEYS):
        same = (line == roll(line, shift)) & (lane % BATCH_KEYS >= shift)
        meet = jnp.where(same, 1.0, meet)
    rows = lax.broadcasted_iota(jnp.int32, (128, 128), 0) // FLAG_KEYS
    shared = (rows == lax.broadcasted_iota(jnp.int32, (128, 128), 1) // FLAG_KEYS).astype(F32)
    ids_ref[0] = line
    ids_ref[1] = jnp.dot(meet, shared, preferred_element_type=F32).astype(jnp.int32)
    group_ref[...] = group.astype(F32).T.astype(jnp.bfloat16)
    return [
        pltpu.make_async_copy(ids_ref.at[0], line_ref, sem.at[0]),
        pltpu.make_async_copy(ids_ref.at[1], flag_ref, sem.at[1]),
    ]


def load_parts(parts, which, scores, sem):
    copies = []
    start = 0
    for i, part in enumerate(parts):
        part = part.at[which] if len(part.shape) == 3 else part
        copies.append(pltpu.make_async_copy(part, scores.at[pl.ds(start, part.shape[0])], sem.at[i]))
        copies[-1].start()
        start += part.shape[0]
    return copies


def clear(hist):
    step = 512

    def body(i, carry):
        hist[pl.ds(pl.multiple_of(i * step, step), step), :] = jnp.zeros((step, 128), F32)
        return carry

    lax.fori_loop(0, hist.shape[0] // step, body, 0)


def across(value, width, combine):
    while width < 128:
        value = combine(value, roll(value, width))
        width *= 2
    return value


def top_of(scores, width):
    step = 512

    def body(i, best):
        block = scores[pl.ds(pl.multiple_of(i * step, step), step), :]
        return jnp.maximum(best, jnp.max(block.reshape(step // 8, 8, 128), axis=0))

    best = lax.fori_loop(0, scores.shape[0] // step, body, jnp.full((8, 128), -jnp.inf, F32))
    return across(jnp.max(best, axis=0, keepdims=True), width, jnp.maximum)


def spread_weights(scores, weights, group_ref, top, width):
    count = 128 // width
    group = lane_group(width)
    spread_lane = lax.broadcasted_iota(jnp.int32, (128, 128), 1) // width
    spread_row = lax.broadcasted_iota(jnp.int32, (128, 128), 0)
    together = 4

    def body(i, total):
        for u in range(together):
            block = i * together + u
            select = (spread_row == block * count + spread_lane).astype(F32).astype(jnp.bfloat16)
            target = jnp.dot(group_ref[...], select, preferred_element_type=F32).astype(jnp.int32)
            shift = (target - group) & (count - 1)
            value = jnp.exp(scores[pl.ds(pl.multiple_of(block * 128, 128), 128), :] - top)
            total = total + jnp.sum(value.reshape(16, 8, 128), axis=0)
            turned = [jnp.where(shift == d, value, 0.0) for d in range(count)]
            turned = [turned[0]] + [roll(turned[d], width * d) for d in range(1, count)]
            for source in range(count):
                line = pick(group, [turned[(g - source) % count] for g in range(count)])
                at = pl.multiple_of((block * count + source) * 128, 128)
                weights[pl.ds(at, 128), :] = line
        return total

    total = lax.fori_loop(0, scores.shape[0] // 128 // together, body, jnp.zeros((8, 128), F32))
    return across(jnp.sum(total, axis=0, keepdims=True), width, jnp.add)


def add_weights(line_ref, flag_ref, weights, hists):
    assert FLAG_KEYS == 128

    def add(hist, row, lane, key, count):
        at = [line_ref[row, lane + k] for k in range(count)]
        sums = [hist[pl.ds(at[k], 1), :] + weights[pl.ds(key + k, 1), :] for k in range(count)]
        for k in range(count):
            hist[pl.ds(at[k], 1), :] = sums[k]

    def body(i, carry):
        key = i * FLAG_KEYS

        def apart():
            for b in range(FLAG_KEYS // BATCH_KEYS):
                add(hists[b % 2], i, b * BATCH_KEYS, key + b * BATCH_KEYS, BATCH_KEYS)

        def one_by_one():
            def step(k, carry):
                for which in range(2):
                    add(hists[which], i, 2 * k + which, key + 2 * k + which, 1)
                return carry

            lax.fori_loop(0, FLAG_KEYS // 2, step, 0)

        lax.cond(flag_ref[i, 0] == 0, apart, one_by_one)
        return carry

    lax.fori_loop(0, weights.shape[0] // FLAG_KEYS, body, 0)


def piece_at(k, size):
    model = lax.axis_index("model")
    x, core = model // 2, model % 2
    x_of = x if k >= 2 else 1 - x
    core_of = core if k % 2 else 1 - core
    return (2 * x_of + core_of) * size


def head_block(top, total):
    row = lax.broadcasted_iota(jnp.int32, (HEAD, 128), 0)
    return jnp.where(row == 0, top, jnp.where(row == 1, total, 0.0))


def own_kernel(which, n_parts, tok_ref, *refs):
    parts, refs = refs[:n_parts], refs[n_parts:]
    outs, refs = refs[:8], refs[8:]
    group_ref, ids_ref, line_ref, flag_ref, id_sem, scores, weights, even, odd, heads, in_sem, out_sem, head_sem = refs
    lines = even.shape[0]
    piece = lines // 8
    copies = load_parts(parts, which, scores, in_sem)
    copies += place_ids(tok_ref, which, group_ref, ids_ref, line_ref, flag_ref, id_sem)
    for copy in copies[-2:]:
        copy.start()
    clear(even)
    clear(odd)
    for copy in copies:
        copy.wait()
    top = top_of(scores, 64)
    total = spread_weights(scores, weights, group_ref, top, 64)
    add_weights(line_ref, flag_ref, weights, (even, odd))

    quad = lane_group(32) % 2 == 0
    tops = [jnp.where(quad, top, roll(top, 32)), jnp.where(quad, roll(top, 32), top)]
    totals = [jnp.where(quad, total, roll(total, 32)), jnp.where(quad, roll(total, 32), total)]
    for c in range(2):
        heads[c] = head_block(tops[c], totals[c])
    together = 5

    sends = []
    for k in range(4):
        base = piece_at(k, 1)

        def split(i, carry, base=base):
            values = []
            for u in range(together):
                block = i * together + u
                near = pl.ds(pl.multiple_of(base * 2 * piece + block * 256, 128), 128)
                far = pl.ds(pl.multiple_of(base * 2 * piece + block * 256 + 128, 128), 128)
                low = even[near, :] + odd[near, :]
                high = roll(even[far, :] + odd[far, :], 32)
                values.append((block, low, high))
            for block, low, high in values:
                weights[pl.ds(pl.multiple_of(base * piece + block * 128, 128), 128), :] = jnp.where(quad, low, high)
                even[pl.ds(pl.multiple_of(base * 2 * piece + block * 128, 128), 128), :] = jnp.where(quad, high, low)
            return carry

        lax.fori_loop(0, piece // 128 // together, split, 0)
        firsts = weights.at[pl.ds(pl.multiple_of(base * piece, 128), piece)]
        seconds = even.at[pl.ds(pl.multiple_of(base * 2 * piece, 128), piece)]
        for c, source in enumerate((firsts, seconds)):
            out = outs[k * 2 + c]
            sends.append(pltpu.make_async_copy(source, out.at[pl.ds(0, piece)], out_sem.at[c, k]))
            sends.append(pltpu.make_async_copy(heads.at[c], out.at[pl.ds(piece, HEAD)], head_sem.at[c, k]))
        for send in sends[-4:]:
            send.start()
    for send in sends:
        send.wait()


def chunk_kernel(which, n_parts, tok_ref, *refs):
    parts, refs = refs[:n_parts], refs[n_parts:]
    prevs, refs = refs[:4], refs[5:]
    outs, refs = refs[:4], refs[4:]
    group_ref, ids_ref, line_ref, flag_ref, id_sem, scores, weights, even, odd, heads, in_sem, *refs = refs
    held, prev_sem, out_sem, head_sem = refs
    lines = even.shape[0]
    piece = lines // 4
    copies = load_parts(parts, which, scores, in_sem)
    fetches = [pltpu.make_async_copy(prevs[k], held.at[k], prev_sem.at[k]) for k in range(4)]
    for fetch in fetches:
        fetch.start()
    copies += place_ids(tok_ref, which, group_ref, ids_ref, line_ref, flag_ref, id_sem)
    for copy in copies[-2:]:
        copy.start()
    clear(even)
    clear(odd)
    for copy in copies:
        copy.wait()
    top = top_of(scores, 32)
    total = spread_weights(scores, weights, group_ref, top, 32)
    add_weights(line_ref, flag_ref, weights, (even, odd))

    for fetch in fetches:
        fetch.wait()
    old_top, old_total = held[0, piece : piece + 1, :], held[0, piece + 1 : piece + 2, :]
    new_top = jnp.maximum(top, old_top)
    scale, old_scale = jnp.exp(top - new_top), jnp.exp(old_top - new_top)
    heads[0] = head_block(new_top, total * scale + old_total * old_scale)
    step = 128
    sends = []
    for k in range(4):
        base = piece_at(k, piece)

        def join(i, carry, base=base, k=k):
            at = pl.ds(pl.multiple_of(base + i * step, step), step)
            old = held[k, pl.ds(pl.multiple_of(i * step, step), step), :]
            even[at, :] = (even[at, :] + odd[at, :]) * scale + old * old_scale
            return carry

        lax.fori_loop(0, piece // step, join, 0)
        source = even.at[pl.ds(pl.multiple_of(base, step), piece)]
        sends.append(pltpu.make_async_copy(source, outs[k].at[pl.ds(0, piece)], out_sem.at[k]))
        sends.append(pltpu.make_async_copy(heads.at[0], outs[k].at[pl.ds(piece, HEAD)], head_sem.at[k]))
        for send in sends[-2:]:
            send.start()
    for send in sends:
        send.wait()


def histogram_call(tok, which, parts, prevs, after, vocab):
    own = not prevs
    rows = sum(part.shape[-2] for part in parts)
    lines = vocab // (2 if own else PACK)
    out = jax.ShapeDtypeStruct((vocab // PACK // 4 + HEAD, 128), F32)
    keys = tok.shape[0]
    tok = tok.reshape(128, 128)
    assert keys == 128 * 128
    count = 8 if own else 4
    dma = pltpu.SemaphoreType.DMA
    extra = [] if own else [*prevs, after]
    return pl.pallas_call(
        functools.partial(own_kernel if own else chunk_kernel, which, len(parts)),
        out_shape=(out,) * count,
        in_specs=[pl.BlockSpec(memory_space=VMEM)]
        + [pl.BlockSpec(memory_space=ANY)] * (len(parts) + len(extra)),
        out_specs=(pl.BlockSpec(memory_space=ANY),) * count,
        scratch_shapes=[VMEM((128, 128), jnp.bfloat16), VMEM((2, 128, 128), jnp.int32)]
        + [SMEM((128, 128), jnp.int32), SMEM((128, 128), jnp.int32), dma((2,))]
        + [VMEM((rows, 128), F32), VMEM((keys, 128), F32), VMEM((lines, 128), F32), VMEM((lines, 128), F32)]
        + [VMEM((2, HEAD, 128), F32), dma((len(parts),))]
        + ([dma((2, 4)), dma((2, 4))] if own else [VMEM((4, lines // 4 + HEAD, 128), F32), dma((4,)), dma((4,)), dma((4,))]),
        compiler_params=pltpu.CompilerParams(vmem_limit_bytes=VMEM_BYTES),
        cost_estimate=pl.CostEstimate(flops=10**6, bytes_accessed=2 * 10**7, transcendentals=0),
        name="own_histogram" if own else "chunk_histogram",
    )(tok, *parts, *extra)


def merge_kernel(a_ref, b_ref, *refs):
    *outs, a_held, b_held, heads, in_sem, out_sem = refs
    lines = a_ref.shape[0] - HEAD
    block = STAGE_BLOCKS * TOK_BLOCK
    steps = lines // block

    def fetch(source, held, which, start, size, index):
        at = pl.ds(start, size)
        return pltpu.make_async_copy(source.at[at], held.at[at], in_sem.at[which, index])

    pairs = [(lines, HEAD)] + [(i * block, block) for i in range(steps)]
    fetches = [
        (fetch(a_ref, a_held, 0, start, size, i), fetch(b_ref, b_held, 1, start, size, i))
        for i, (start, size) in enumerate(pairs)
    ]
    for pair in fetches:
        for copy in pair:
            copy.start()
    sends = []
    for i, (start, size) in enumerate(pairs):
        for copy in fetches[i]:
            copy.wait()
        if i == 0:
            a_top, b_top = a_held[lines : lines + 1, :], b_held[lines : lines + 1, :]
            top = jnp.maximum(a_top, b_top)
            a_scale, b_scale = jnp.exp(a_top - top), jnp.exp(b_top - top)
            total = a_held[lines + 1 : lines + 2, :] * a_scale + b_held[lines + 1 : lines + 2, :] * b_scale
            heads[...] = head_block(top, total)
            source = heads
        else:
            at = slice(start, start + size)
            a_held[at, :] = a_held[at, :] * a_scale + b_held[at, :] * b_scale
            source = a_held.at[pl.ds(start, size)]
        if len(outs) == 1:
            target = outs[0].at[pl.ds(start, size)]
        else:
            first = outs[0].shape[0]
            target = outs[0].at[pl.ds(start, size)] if start < first else outs[1].at[pl.ds(start - first, size)]
        sends.append(pltpu.make_async_copy(source, target, out_sem.at[i]))
        sends[-1].start()
    for send in sends:
        send.wait()


def merge_call(a, b, parted):
    block = STAGE_BLOCKS * TOK_BLOCK
    steps = a.shape[0] // block
    sizes = (a.shape[0] - HEAD - block, block + HEAD) if parted else (a.shape[0],)
    dma = pltpu.SemaphoreType.DMA
    return pl.pallas_call(
        merge_kernel,
        out_shape=tuple(jax.ShapeDtypeStruct((size, 128), F32) for size in sizes),
        in_specs=[pl.BlockSpec(memory_space=ANY)] * 2,
        out_specs=tuple(pl.BlockSpec(memory_space=ANY) for _ in sizes),
        scratch_shapes=[VMEM(a.shape, F32), VMEM(a.shape, F32), VMEM((HEAD, 128), F32), dma((2, steps + 1)), dma((steps + 1,))],
        compiler_params=pltpu.CompilerParams(vmem_limit_bytes=VMEM_BYTES),
        cost_estimate=pl.CostEstimate(flops=10**5, bytes_accessed=3 * a.size * 4, transcendentals=0),
        name="merge",
    )(a, b)


def head_kernel(q_ref, w_ref, after_ref, logits_ref, stat_ref, top_ref, sum_ref):
    del after_ref
    i = pl.program_id(0)

    @pl.when(i == 0)
    def _():
        top_ref[...] = jnp.full(top_ref.shape, -jnp.inf, F32)
        sum_ref[...] = jnp.zeros(sum_ref.shape, F32)

    rows = logits_ref.shape[0]
    mine = q_ref[pl.ds(pl.multiple_of(lax.axis_index("store") * rows, rows), rows), :]
    logits = jnp.dot(mine, w_ref[...], preferred_element_type=F32)
    logits_ref[...] = logits
    old = top_ref[...]
    new = jnp.maximum(old, jnp.max(logits, axis=1, keepdims=True))
    part = jnp.sum(jnp.exp(logits - new[:, 0:1]), axis=1, keepdims=True)
    sum_ref[...] = sum_ref[...] * jnp.exp(old - new) + part
    top_ref[...] = new
    stat_ref[0] = top_ref[...]
    stat_ref[1] = sum_ref[...]


def head_call(queries, w_head, after):
    width = queries.shape[1]
    count = queries.shape[0] // 2
    cols = w_head.shape[1]
    block = cols // 10
    return pl.pallas_call(
        head_kernel,
        grid=(cols // block,),
        out_shape=(jax.ShapeDtypeStruct((count, cols), F32), jax.ShapeDtypeStruct((2, count, 128), F32)),
        in_specs=[
            pl.BlockSpec((2 * count, width), lambda i: (0, 0)),
            pl.BlockSpec((width, block), lambda i: (0, i)),
            pl.BlockSpec(memory_space=ANY),
        ],
        out_specs=(pl.BlockSpec((count, block), lambda i: (0, i)), pl.BlockSpec((2, count, 128), lambda i: (0, 0, 0))),
        scratch_shapes=[VMEM((count, 128), F32), VMEM((count, 128), F32)],
        compiler_params=pltpu.CompilerParams(vmem_limit_bytes=VMEM_BYTES),
        cost_estimate=pl.CostEstimate(flops=2 * count * width * cols, bytes_accessed=2 * width * cols, transcendentals=0),
        name="head",
    )(queries, w_head, after)


def mix_kernel(index, n_far, n_prev, mix_ref, stat_ref, logits_ref, *refs):
    pieces, refs = refs[: 2 + n_far], refs[2 + n_far + n_prev :]
    out_ref, held, heads, logits, result, in_sem, head_sem, logits_sem, out_sem = refs
    order = ORDERS[index]
    block = STAGE_BLOCKS * TOK_BLOCK
    steps = held.shape[1] // block
    wide = block * PACK
    rows = pl.ds(index * 32, 32)

    def sources(start, size):
        first = pieces[2].shape[0]
        far = pieces[2].at[pl.ds(start, size)] if start < first else pieces[3].at[pl.ds(start - first, size)]
        return [pieces[0].at[pl.ds(start, size)], pieces[1].at[pl.ds(start, size)], far]

    head_copies = [
        pltpu.make_async_copy(source, heads.at[p], head_sem.at[p])
        for p, source in enumerate(sources(steps * block, HEAD))
    ]
    for copy in head_copies:
        copy.start()
    copies = []
    for i in range(steps):
        at = pl.ds(i * block, block)
        cols = pl.ds(i * wide, wide)
        group = [
            pltpu.make_async_copy(source, held.at[p, at], in_sem.at[i, p])
            for p, source in enumerate(sources(i * block, block))
        ]
        group.append(pltpu.make_async_copy(logits_ref.at[rows, cols], logits.at[:, cols], logits_sem.at[i]))
        for copy in group:
            copy.start()
        copies.append(group)
    for copy in head_copies:
        copy.wait()
    mix = mix_ref[0]
    tops = [heads[p, 0:1, :] for p in range(3)]
    top = jnp.maximum(jnp.maximum(tops[0], tops[1]), tops[2])
    scales = [jnp.exp(value - top) for value in tops]
    total = sum(heads[p, 1:2, :] * scales[p] for p in range(3))
    scales = [scale * mix / total for scale in scales]
    lm_top = stat_ref[0, index * 32 : index * 32 + 32, :]
    lm_scale = (1.0 - mix) / stat_ref[1, index * 32 : index * 32 + 32, :]
    sends = []
    for i in range(steps):
        for copy in copies[i]:
            copy.wait()
        for b in range(i * STAGE_BLOCKS, (i + 1) * STAGE_BLOCKS):
            at = slice(b * TOK_BLOCK, (b + 1) * TOK_BLOCK)
            turned = sum(held[p, at, :] * scales[p] for p in range(3)).T
            for g in range(PACK):
                run = order[g]
                cols = slice((b * PACK + run) * TOK_BLOCK, (b * PACK + run + 1) * TOK_BLOCK)
                lm = jnp.exp(logits[:, cols] - lm_top) * lm_scale
                result[:, cols] = jnp.log(turned[g * 32 : (g + 1) * 32, :] + lm)
        cols = pl.ds(i * wide, wide)
        sends.append(pltpu.make_async_copy(result.at[:, cols], out_ref.at[rows, cols], out_sem.at[i]))
        sends[-1].start()
    for send in sends:
        send.wait()


def mix_call(mix, pieces, logits, stat, index, prev):
    lines = pieces[0].shape[0] - HEAD
    steps = lines // (STAGE_BLOCKS * TOK_BLOCK)
    count, cols = logits.shape
    n_prev = 0 if prev is None else 1
    dma = pltpu.SemaphoreType.DMA
    return pl.pallas_call(
        functools.partial(mix_kernel, index, len(pieces) - 2, n_prev),
        out_shape=jax.ShapeDtypeStruct((count, cols), F32),
        in_specs=[pl.BlockSpec(memory_space=SMEM), pl.BlockSpec(memory_space=VMEM)]
        + [pl.BlockSpec(memory_space=ANY)] * (1 + len(pieces) + n_prev),
        out_specs=pl.BlockSpec(memory_space=ANY),
        scratch_shapes=[VMEM((3, lines, 128), F32), VMEM((3, HEAD, 128), F32), VMEM((32, cols), F32), VMEM((32, cols), F32)]
        + [dma((steps, 3)), dma((3,)), dma((steps,)), dma((steps,))],
        input_output_aliases={3 + len(pieces): 0} if n_prev else {},
        compiler_params=pltpu.CompilerParams(vmem_limit_bytes=VMEM_BYTES),
        cost_estimate=pl.CostEstimate(flops=10**5, bytes_accessed=8 * 10**6, transcendentals=0),
        name="mix",
    )(mix, stat, logits, *pieces, *([prev] if n_prev else []))


CHUNKS = (5120, 11264)


def solution(mesh):
    store_devs = mesh.shape["store"]
    model_devs = mesh.shape["model"]
    assert store_devs == 2 and model_devs == 4
    group_axes = ("store", "model")
    across_y = [(0, 1), (1, 0)]
    across_core = [(0, 1), (1, 0), (2, 3), (3, 2)]
    across_x = [(0, 2), (2, 0), (1, 3), (3, 1)]

    def swap_y(value):
        return lax.ppermute(value, "store", across_y)

    def swap_core(value):
        return lax.ppermute(value, "model", across_core)

    def swap_x(value):
        return lax.ppermute(value, "model", across_x)

    def local_step(queries, w_head, store_keys, store_tok, temperature, mix_weight):
        vocab = w_head.shape[1] * model_devs
        tau = temperature.reshape(1)
        mix = mix_weight.reshape(1)

        their_tok = swap_y(store_tok)
        own, first, second = [], [], []
        start = 0
        for index, count in enumerate(CHUNKS):
            joined = index == 0
            kept, *sent = score_call(tau, queries, store_keys, start, count, joined)
            own.append(kept)
            first.append(swap_y(sent[0]))
            if joined:
                second.append(first[-1])
            else:
                second.append(swap_y(sent[1]))
            start += count

        kept = histogram_call(store_tok, None, own, [], None, vocab)
        nears, fars = [], []
        after = kept[0]
        for index, parts in enumerate((first, second)):
            out = histogram_call(their_tok, index, parts, kept[index::2], after, vocab)
            far = swap_core(out[0])
            near = swap_core(out[2])
            sums = merge_call(out[1], far, index == 1)
            if index == 0:
                after = sums[0]
                fars.append([swap_x(sums[0])])
            else:
                fars.append([swap_x(sums[0])])
            nears.append([out[3], near])
        logits, stat = head_call(queries, w_head, sums[0])
        for swap in (swap_core, swap_x):
            other = swap(stat)
            top = jnp.maximum(stat[0], other[0])
            stat = jnp.stack([top, stat[1] * jnp.exp(stat[0] - top) + other[1] * jnp.exp(other[0] - top)])
        fars[1].append(swap_x(sums[1]))
        result = None
        for index in range(2):
            result = mix_call(mix, nears[index] + fars[index], logits, stat, index, result)
        return result

    return jax.shard_map(
        local_step,
        mesh=mesh,
        in_specs=(P("data", None), P(None, "model"), P(group_axes, None), P(group_axes), P(), P()),
        out_specs=P(("data", "store"), "model"),
        check_vma=False,
    )
```

```python
import functools

import jax
import jax.numpy as jnp
from jax import lax
from jax.experimental import pallas as pl
from jax.experimental.pallas import tpu as pltpu
from jax.sharding import PartitionSpec as P


F32 = jnp.float32
ANY = pl.ANY
VMEM = pltpu.VMEM
SMEM = pltpu.SMEM
KEY_BLOCK = 1024
LANES = 128
VMEM_BYTES = 63 * 2**20
BATCH_KEYS = 8
FLAG_KEYS = 32
STEP_ROWS = 2
PACK = 4
TOK_BLOCK = 128
ORDERS = ((0, 2, 1, 3), (3, 0, 2, 1))
STAGE_BLOCKS = 5
HEAD = 8


def lane_group(width):
    return lax.broadcasted_iota(jnp.int32, (1, LANES), 1) // width


def pick(group, parts):
    out = parts[-1]
    for index in range(len(parts) - 2, -1, -1):
        out = jnp.where(group == index, parts[index], out)
    return out


def roll(value, shift):
    return pltpu.roll(value, shift % LANES, 1)


def score_kernel(tau_ref, rows_ref, k_ref, own_ref, *sent):
    *sent, q_ref = sent
    tau = tau_ref[0]
    first_ref, second_ref = (sent[0].at[0], sent[0].at[1]) if len(sent) == 1 else sent

    @pl.when(pl.program_id(0) == 0)
    def _():
        half = q_ref.shape[0] // 2
        y = lax.axis_index("store")
        q_ref[0:half, :] = rows_ref[pl.ds(pl.multiple_of(y * half, half), half), :]
        q_ref[half : 2 * half, :] = rows_ref[pl.ds(pl.multiple_of((1 - y) * half, half), half), :]

    dots = lax.dot_general(k_ref[...], q_ref[...], (((1,), (1,)), ((), ())), preferred_element_type=F32)
    step = LANES
    norms = []
    for row in range(0, KEY_BLOCK, step):
        acc = jnp.zeros((step, LANES), F32)
        for col in range(0, k_ref.shape[1], LANES):
            part = k_ref[row : row + step, col : col + LANES].astype(F32)
            acc += part * part
        norms.append(jnp.sum(acc, axis=1, keepdims=True))
    group = lane_group(32)
    scores = [(2.0 * dots[i * step : (i + 1) * step] - norms[i]) / tau for i in range(KEY_BLOCK // step)]
    for i in range(KEY_BLOCK // step // 2):
        own_ref[i * step : (i + 1) * step, :] = jnp.where(group < 2, scores[2 * i], roll(scores[2 * i + 1], 64))
    for i in range(KEY_BLOCK // step // 4):
        four = scores[4 * i : 4 * i + 4]
        rows = slice(i * step, (i + 1) * step)
        first_ref[rows, :] = pick(group, [roll(four[0], 64), roll(four[1], 96), four[2], roll(four[3], 32)])
        second_ref[rows, :] = pick(group, [roll(four[0], 32), roll(four[1], 64), roll(four[2], 96), four[3]])


def score_call(tau, queries, keys, start, count, joined):
    width = keys.shape[1]
    base = start // KEY_BLOCK
    half, quarter = KEY_BLOCK // 2, KEY_BLOCK // 4
    if joined:
        sent_shape = (jax.ShapeDtypeStruct((2, count // 4, LANES), F32),)
        sent_spec = (pl.BlockSpec((2, quarter, LANES), lambda i: (0, i, 0)),)
    else:
        sent_shape = (jax.ShapeDtypeStruct((count // 4, LANES), F32),) * 2
        sent_spec = (pl.BlockSpec((quarter, LANES), lambda i: (i, 0)),) * 2
    return pl.pallas_call(
        score_kernel,
        grid=(count // KEY_BLOCK,),
        out_shape=(jax.ShapeDtypeStruct((count // 2, LANES), F32),) + sent_shape,
        in_specs=[
            pl.BlockSpec(memory_space=SMEM),
            pl.BlockSpec((LANES, width), lambda i: (0, 0)),
            pl.BlockSpec((KEY_BLOCK, width), lambda i: (i + base, 0)),
        ],
        out_specs=(pl.BlockSpec((half, LANES), lambda i: (i, 0)),) + sent_spec,
        scratch_shapes=[VMEM((LANES, width), jnp.bfloat16)],
        compiler_params=pltpu.CompilerParams(vmem_limit_bytes=VMEM_BYTES),
        cost_estimate=pl.CostEstimate(flops=2 * count * width * LANES, bytes_accessed=2 * count * width, transcendentals=0),
        name="scores",
    )(tau, queries, keys)


def place_ids(tok_ref, which, group_ref, ids_ref, line_ref, flag_ref, sem):
    assert PACK == 4 and TOK_BLOCK == LANES
    tok = tok_ref[...]
    block, run, within = tok >> 9, (tok >> 7) & 3, tok & 127
    if which is None:
        line = block * 256 + (run >> 1) * LANES + within
        group = run & 1
    else:
        line = block * LANES + within
        group = sum(jnp.where(run == ORDERS[which][g], g, 0) for g in range(PACK))
    lane = lax.broadcasted_iota(jnp.int32, (1, LANES), 1)
    meet = jnp.zeros(tok.shape, F32)
    for shift in range(1, BATCH_KEYS):
        same = (line == roll(line, shift)) & (lane % BATCH_KEYS >= shift)
        meet = jnp.where(same, 1.0, meet)
    rows = lax.broadcasted_iota(jnp.int32, (LANES, LANES), 0) // FLAG_KEYS
    shared = (rows == lax.broadcasted_iota(jnp.int32, (LANES, LANES), 1) // FLAG_KEYS).astype(F32)
    ids_ref[0] = line
    ids_ref[1] = jnp.dot(meet, shared, preferred_element_type=F32).astype(jnp.int32)
    group_ref[...] = group.astype(F32).T.astype(jnp.bfloat16)
    return [
        pltpu.make_async_copy(ids_ref.at[0], line_ref, sem.at[0]),
        pltpu.make_async_copy(ids_ref.at[1], flag_ref, sem.at[1]),
    ]


def load_parts(parts, which, scores, sem):
    copies = []
    start = 0
    for i, part in enumerate(parts):
        part = part.at[which] if len(part.shape) == 3 else part
        copies.append(pltpu.make_async_copy(part, scores.at[pl.ds(start, part.shape[0])], sem.at[i]))
        copies[-1].start()
        start += part.shape[0]
    return copies


def clear(hist):
    step = 512

    def body(i, carry):
        hist[pl.ds(pl.multiple_of(i * step, step), step), :] = jnp.zeros((step, LANES), F32)
        return carry

    lax.fori_loop(0, hist.shape[0] // step, body, 0)


def across(value, width, combine):
    while width < LANES:
        value = combine(value, roll(value, width))
        width *= 2
    return value


def top_of(scores, width):
    step = 512

    def body(i, best):
        block = scores[pl.ds(pl.multiple_of(i * step, step), step), :]
        return jnp.maximum(best, jnp.max(block.reshape(step // 8, 8, LANES), axis=0))

    best = lax.fori_loop(0, scores.shape[0] // step, body, jnp.full((8, LANES), -jnp.inf, F32))
    return across(jnp.max(best, axis=0, keepdims=True), width, jnp.maximum)


def spread_weights(scores, weights, group_ref, top, width):
    count = LANES // width
    group = lane_group(width)
    spread_lane = lax.broadcasted_iota(jnp.int32, (LANES, LANES), 1) // width
    spread_row = lax.broadcasted_iota(jnp.int32, (LANES, LANES), 0)
    together = 4

    def body(i, total):
        for u in range(together):
            block = i * together + u
            select = (spread_row == block * count + spread_lane).astype(F32).astype(jnp.bfloat16)
            target = jnp.dot(group_ref[...], select, preferred_element_type=F32).astype(jnp.int32)
            shift = (target - group) & (count - 1)
            value = jnp.exp(scores[pl.ds(pl.multiple_of(block * LANES, LANES), LANES), :] - top)
            total = total + jnp.sum(value.reshape(16, 8, LANES), axis=0)
            turned = [jnp.where(shift == d, value, 0.0) for d in range(count)]
            turned = [turned[0]] + [roll(turned[d], width * d) for d in range(1, count)]
            for source in range(count):
                line = pick(group, [turned[(g - source) % count] for g in range(count)])
                at = pl.multiple_of((block * count + source) * LANES, LANES)
                weights[pl.ds(at, LANES), :] = line
        return total

    total = lax.fori_loop(0, scores.shape[0] // LANES // together, body, jnp.zeros((8, LANES), F32))
    return across(jnp.sum(total, axis=0, keepdims=True), width, jnp.add)


def add_weights(line_ref, flag_ref, weights, hists):
    def add(hist, row, lane, key, count):
        at = [line_ref[row, lane + k] for k in range(count)]
        sums = [hist[pl.ds(at[k], 1), :] + weights[pl.ds(key + k, 1), :] for k in range(count)]
        for k in range(count):
            hist[pl.ds(at[k], 1), :] = sums[k]

    def body(i, carry):
        first = i * STEP_ROWS
        groups = [(r, lane) for r in range(STEP_ROWS) for lane in range(0, LANES, FLAG_KEYS)]
        flags = [flag_ref[first + r, lane] for r, lane in groups]

        def apart(r, lane, count):
            for b in range(count // BATCH_KEYS):
                at = lane + b * BATCH_KEYS
                add(hists[b % 2], first + r, at, (first + r) * LANES + at, BATCH_KEYS)

        def one_by_one(r, lane):
            def step(k, carry):
                for which in range(2):
                    at = lane + 2 * k + which
                    add(hists[which], first + r, at, (first + r) * LANES + at, 1)
                return carry

            lax.fori_loop(0, FLAG_KEYS // 2, step, 0)

        def all_apart():
            for r in range(STEP_ROWS):
                apart(r, 0, LANES)

        def some_apart():
            for (r, lane), flag in zip(groups, flags):
                lax.cond(flag == 0, lambda: apart(r, lane, FLAG_KEYS), lambda: one_by_one(r, lane))

        lax.cond(sum(flags) == 0, all_apart, some_apart)
        return carry

    lax.fori_loop(0, weights.shape[0] // LANES // STEP_ROWS, body, 0)


def piece_at(k, size):
    model = lax.axis_index("model")
    x, core = model // 2, model % 2
    x_of = x if k >= 2 else 1 - x
    core_of = core if k % 2 else 1 - core
    return (2 * x_of + core_of) * size


def head_block(top, total):
    row = lax.broadcasted_iota(jnp.int32, (HEAD, LANES), 0)
    return jnp.where(row == 0, top, jnp.where(row == 1, total, 0.0))


def own_kernel(which, n_parts, tok_ref, *refs):
    parts, refs = refs[:n_parts], refs[n_parts:]
    outs, refs = refs[:8], refs[8:]
    group_ref, ids_ref, line_ref, flag_ref, id_sem, scores, weights, even, odd, heads, in_sem, out_sem, head_sem = refs
    lines = even.shape[0]
    piece = lines // 8
    copies = load_parts(parts, which, scores, in_sem)
    copies += place_ids(tok_ref, which, group_ref, ids_ref, line_ref, flag_ref, id_sem)
    for copy in copies[-2:]:
        copy.start()
    clear(even)
    clear(odd)
    for copy in copies:
        copy.wait()
    top = top_of(scores, 64)
    total = spread_weights(scores, weights, group_ref, top, 64)
    add_weights(line_ref, flag_ref, weights, (even, odd))

    quad = lane_group(32) % 2 == 0
    tops = [jnp.where(quad, top, roll(top, 32)), jnp.where(quad, roll(top, 32), top)]
    totals = [jnp.where(quad, total, roll(total, 32)), jnp.where(quad, roll(total, 32), total)]
    for c in range(2):
        heads[c] = head_block(tops[c], totals[c])
    together = 5

    sends = []
    for k in range(4):
        base = piece_at(k, 1)

        def split(i, carry, base=base):
            values = []
            for u in range(together):
                block = i * together + u
                near = pl.ds(pl.multiple_of(base * 2 * piece + block * 256, LANES), LANES)
                far = pl.ds(pl.multiple_of(base * 2 * piece + block * 256 + LANES, LANES), LANES)
                low = even[near, :] + odd[near, :]
                high = roll(even[far, :] + odd[far, :], 32)
                values.append((block, low, high))
            for block, low, high in values:
                weights[pl.ds(pl.multiple_of(base * piece + block * LANES, LANES), LANES), :] = jnp.where(quad, low, high)
                even[pl.ds(pl.multiple_of(base * 2 * piece + block * LANES, LANES), LANES), :] = jnp.where(quad, high, low)
            return carry

        lax.fori_loop(0, piece // LANES // together, split, 0)
        firsts = weights.at[pl.ds(pl.multiple_of(base * piece, LANES), piece)]
        seconds = even.at[pl.ds(pl.multiple_of(base * 2 * piece, LANES), piece)]
        for c, source in enumerate((firsts, seconds)):
            out = outs[k * 2 + c]
            sends.append(pltpu.make_async_copy(source, out.at[pl.ds(0, piece)], out_sem.at[c, k]))
            sends.append(pltpu.make_async_copy(heads.at[c], out.at[pl.ds(piece, HEAD)], head_sem.at[c, k]))
        for send in sends[-4:]:
            send.start()
    for send in sends:
        send.wait()


def chunk_kernel(which, n_parts, tok_ref, *refs):
    parts, refs = refs[:n_parts], refs[n_parts:]
    prevs, refs = refs[:4], refs[5:]
    outs, refs = refs[:4], refs[4:]
    group_ref, ids_ref, line_ref, flag_ref, id_sem, scores, weights, even, odd, heads, in_sem, *refs = refs
    held, prev_sem, out_sem, head_sem = refs
    lines = even.shape[0]
    piece = lines // 4
    copies = load_parts(parts, which, scores, in_sem)
    fetches = [pltpu.make_async_copy(prevs[k], held.at[k], prev_sem.at[k]) for k in range(4)]
    for fetch in fetches:
        fetch.start()
    copies += place_ids(tok_ref, which, group_ref, ids_ref, line_ref, flag_ref, id_sem)
    for copy in copies[-2:]:
        copy.start()
    clear(even)
    clear(odd)
    for copy in copies:
        copy.wait()
    top = top_of(scores, 32)
    total = spread_weights(scores, weights, group_ref, top, 32)
    add_weights(line_ref, flag_ref, weights, (even, odd))

    for fetch in fetches:
        fetch.wait()
    old_top, old_total = held[0, piece : piece + 1, :], held[0, piece + 1 : piece + 2, :]
    new_top = jnp.maximum(top, old_top)
    scale, old_scale = jnp.exp(top - new_top), jnp.exp(old_top - new_top)
    heads[0] = head_block(new_top, total * scale + old_total * old_scale)
    step = LANES
    sends = []
    for k in range(4):
        base = piece_at(k, piece)

        def join(i, carry, base=base, k=k):
            at = pl.ds(pl.multiple_of(base + i * step, step), step)
            old = held[k, pl.ds(pl.multiple_of(i * step, step), step), :]
            even[at, :] = (even[at, :] + odd[at, :]) * scale + old * old_scale
            return carry

        lax.fori_loop(0, piece // step, join, 0)
        source = even.at[pl.ds(pl.multiple_of(base, step), piece)]
        sends.append(pltpu.make_async_copy(source, outs[k].at[pl.ds(0, piece)], out_sem.at[k]))
        sends.append(pltpu.make_async_copy(heads.at[0], outs[k].at[pl.ds(piece, HEAD)], head_sem.at[k]))
        for send in sends[-2:]:
            send.start()
    for send in sends:
        send.wait()


def histogram_call(tok, which, parts, prevs, after, vocab):
    own = not prevs
    rows = sum(part.shape[-2] for part in parts)
    lines = vocab // (2 if own else PACK)
    out = jax.ShapeDtypeStruct((vocab // PACK // 4 + HEAD, LANES), F32)
    keys = tok.shape[0]
    tok = tok.reshape(LANES, LANES)
    assert keys == LANES * LANES
    count = 8 if own else 4
    dma = pltpu.SemaphoreType.DMA
    extra = [] if own else [*prevs, after]
    return pl.pallas_call(
        functools.partial(own_kernel if own else chunk_kernel, which, len(parts)),
        out_shape=(out,) * count,
        in_specs=[pl.BlockSpec(memory_space=VMEM)]
        + [pl.BlockSpec(memory_space=ANY)] * (len(parts) + len(extra)),
        out_specs=(pl.BlockSpec(memory_space=ANY),) * count,
        scratch_shapes=[VMEM((LANES, LANES), jnp.bfloat16), VMEM((2, LANES, LANES), jnp.int32)]
        + [SMEM((LANES, LANES), jnp.int32), SMEM((LANES, LANES), jnp.int32), dma((2,))]
        + [VMEM((rows, LANES), F32), VMEM((keys, LANES), F32), VMEM((lines, LANES), F32), VMEM((lines, LANES), F32)]
        + [VMEM((2, HEAD, LANES), F32), dma((len(parts),))]
        + ([dma((2, 4)), dma((2, 4))] if own else [VMEM((4, lines // 4 + HEAD, LANES), F32), dma((4,)), dma((4,)), dma((4,))]),
        compiler_params=pltpu.CompilerParams(vmem_limit_bytes=VMEM_BYTES),
        cost_estimate=pl.CostEstimate(flops=10**6, bytes_accessed=2 * 10**7, transcendentals=0),
        name="own_histogram" if own else "chunk_histogram",
    )(tok, *parts, *extra)


def merge_kernel(a_ref, b_ref, *refs):
    *outs, a_held, b_held, heads, in_sem, out_sem = refs
    lines = a_ref.shape[0] - HEAD
    block = STAGE_BLOCKS * TOK_BLOCK
    steps = lines // block

    def fetch(source, held, which, start, size, index):
        at = pl.ds(start, size)
        return pltpu.make_async_copy(source.at[at], held.at[at], in_sem.at[which, index])

    pairs = [(lines, HEAD)] + [(i * block, block) for i in range(steps)]
    fetches = [
        (fetch(a_ref, a_held, 0, start, size, i), fetch(b_ref, b_held, 1, start, size, i))
        for i, (start, size) in enumerate(pairs)
    ]
    for pair in fetches:
        for copy in pair:
            copy.start()
    sends = []
    for i, (start, size) in enumerate(pairs):
        for copy in fetches[i]:
            copy.wait()
        if i == 0:
            a_top, b_top = a_held[lines : lines + 1, :], b_held[lines : lines + 1, :]
            top = jnp.maximum(a_top, b_top)
            a_scale, b_scale = jnp.exp(a_top - top), jnp.exp(b_top - top)
            total = a_held[lines + 1 : lines + 2, :] * a_scale + b_held[lines + 1 : lines + 2, :] * b_scale
            heads[...] = head_block(top, total)
            source = heads
        else:
            at = slice(start, start + size)
            a_held[at, :] = a_held[at, :] * a_scale + b_held[at, :] * b_scale
            source = a_held.at[pl.ds(start, size)]
        if len(outs) == 1:
            target = outs[0].at[pl.ds(start, size)]
        else:
            first = outs[0].shape[0]
            target = outs[0].at[pl.ds(start, size)] if start < first else outs[1].at[pl.ds(start - first, size)]
        sends.append(pltpu.make_async_copy(source, target, out_sem.at[i]))
        sends[-1].start()
    for send in sends:
        send.wait()


def merge_call(a, b, parted):
    block = STAGE_BLOCKS * TOK_BLOCK
    steps = a.shape[0] // block
    sizes = (a.shape[0] - HEAD - block, block + HEAD) if parted else (a.shape[0],)
    dma = pltpu.SemaphoreType.DMA
    return pl.pallas_call(
        merge_kernel,
        out_shape=tuple(jax.ShapeDtypeStruct((size, LANES), F32) for size in sizes),
        in_specs=[pl.BlockSpec(memory_space=ANY)] * 2,
        out_specs=tuple(pl.BlockSpec(memory_space=ANY) for _ in sizes),
        scratch_shapes=[VMEM(a.shape, F32), VMEM(a.shape, F32), VMEM((HEAD, LANES), F32), dma((2, steps + 1)), dma((steps + 1,))],
        compiler_params=pltpu.CompilerParams(vmem_limit_bytes=VMEM_BYTES),
        cost_estimate=pl.CostEstimate(flops=10**5, bytes_accessed=3 * a.size * 4, transcendentals=0),
        name="merge",
    )(a, b)


def head_kernel(q_ref, w_ref, after_ref, logits_ref, stat_ref, top_ref, sum_ref):
    del after_ref
    i = pl.program_id(0)

    @pl.when(i == 0)
    def _():
        top_ref[...] = jnp.full(top_ref.shape, -jnp.inf, F32)
        sum_ref[...] = jnp.zeros(sum_ref.shape, F32)

    rows = logits_ref.shape[0]
    mine = q_ref[pl.ds(pl.multiple_of(lax.axis_index("store") * rows, rows), rows), :]
    logits = jnp.dot(mine, w_ref[...], preferred_element_type=F32)
    logits_ref[...] = logits
    old = top_ref[...]
    new = jnp.maximum(old, jnp.max(logits, axis=1, keepdims=True))
    part = jnp.sum(jnp.exp(logits - new[:, 0:1]), axis=1, keepdims=True)
    sum_ref[...] = sum_ref[...] * jnp.exp(old - new) + part
    top_ref[...] = new
    stat_ref[0] = top_ref[...]
    stat_ref[1] = sum_ref[...]


def head_call(queries, w_head, after):
    width = queries.shape[1]
    count = queries.shape[0] // 2
    cols = w_head.shape[1]
    block = cols // 10
    return pl.pallas_call(
        head_kernel,
        grid=(cols // block,),
        out_shape=(jax.ShapeDtypeStruct((count, cols), F32), jax.ShapeDtypeStruct((2, count, LANES), F32)),
        in_specs=[
            pl.BlockSpec((2 * count, width), lambda i: (0, 0)),
            pl.BlockSpec((width, block), lambda i: (0, i)),
            pl.BlockSpec(memory_space=ANY),
        ],
        out_specs=(pl.BlockSpec((count, block), lambda i: (0, i)), pl.BlockSpec((2, count, LANES), lambda i: (0, 0, 0))),
        scratch_shapes=[VMEM((count, LANES), F32), VMEM((count, LANES), F32)],
        compiler_params=pltpu.CompilerParams(vmem_limit_bytes=VMEM_BYTES),
        cost_estimate=pl.CostEstimate(flops=2 * count * width * cols, bytes_accessed=2 * width * cols, transcendentals=0),
        name="head",
    )(queries, w_head, after)


def mix_kernel(index, n_far, n_prev, mix_ref, stat_ref, logits_ref, *refs):
    pieces, refs = refs[: 2 + n_far], refs[2 + n_far + n_prev :]
    out_ref, held, heads, logits, result, in_sem, head_sem, logits_sem, out_sem = refs
    order = ORDERS[index]
    block = STAGE_BLOCKS * TOK_BLOCK
    steps = held.shape[1] // block
    wide = block * PACK
    rows = pl.ds(index * 32, 32)

    def sources(start, size):
        first = pieces[2].shape[0]
        far = pieces[2].at[pl.ds(start, size)] if start < first else pieces[3].at[pl.ds(start - first, size)]
        return [pieces[0].at[pl.ds(start, size)], pieces[1].at[pl.ds(start, size)], far]

    head_copies = [
        pltpu.make_async_copy(source, heads.at[p], head_sem.at[p])
        for p, source in enumerate(sources(steps * block, HEAD))
    ]
    for copy in head_copies:
        copy.start()
    copies = []
    for i in range(steps):
        at = pl.ds(i * block, block)
        cols = pl.ds(i * wide, wide)
        group = [
            pltpu.make_async_copy(source, held.at[p, at], in_sem.at[i, p])
            for p, source in enumerate(sources(i * block, block))
        ]
        group.append(pltpu.make_async_copy(logits_ref.at[rows, cols], logits.at[:, cols], logits_sem.at[i]))
        for copy in group:
            copy.start()
        copies.append(group)
    for copy in head_copies:
        copy.wait()
    mix = mix_ref[0]
    tops = [heads[p, 0:1, :] for p in range(3)]
    top = jnp.maximum(jnp.maximum(tops[0], tops[1]), tops[2])
    scales = [jnp.exp(value - top) for value in tops]
    total = sum(heads[p, 1:2, :] * scales[p] for p in range(3))
    scales = [scale * mix / total for scale in scales]
    lm_top = stat_ref[0, index * 32 : index * 32 + 32, :]
    lm_scale = (1.0 - mix) / stat_ref[1, index * 32 : index * 32 + 32, :]
    sends = []
    for i in range(steps):
        for copy in copies[i]:
            copy.wait()
        for b in range(i * STAGE_BLOCKS, (i + 1) * STAGE_BLOCKS):
            at = slice(b * TOK_BLOCK, (b + 1) * TOK_BLOCK)
            turned = sum(held[p, at, :] * scales[p] for p in range(3)).T
            for g in range(PACK):
                run = order[g]
                cols = slice((b * PACK + run) * TOK_BLOCK, (b * PACK + run + 1) * TOK_BLOCK)
                lm = jnp.exp(logits[:, cols] - lm_top) * lm_scale
                result[:, cols] = jnp.log(turned[g * 32 : (g + 1) * 32, :] + lm)
        cols = pl.ds(i * wide, wide)
        sends.append(pltpu.make_async_copy(result.at[:, cols], out_ref.at[rows, cols], out_sem.at[i]))
        sends[-1].start()
    for send in sends:
        send.wait()


def mix_call(mix, pieces, logits, stat, index, prev):
    lines = pieces[0].shape[0] - HEAD
    steps = lines // (STAGE_BLOCKS * TOK_BLOCK)
    count, cols = logits.shape
    n_prev = 0 if prev is None else 1
    dma = pltpu.SemaphoreType.DMA
    return pl.pallas_call(
        functools.partial(mix_kernel, index, len(pieces) - 2, n_prev),
        out_shape=jax.ShapeDtypeStruct((count, cols), F32),
        in_specs=[pl.BlockSpec(memory_space=SMEM), pl.BlockSpec(memory_space=VMEM)]
        + [pl.BlockSpec(memory_space=ANY)] * (1 + len(pieces) + n_prev),
        out_specs=pl.BlockSpec(memory_space=ANY),
        scratch_shapes=[VMEM((3, lines, LANES), F32), VMEM((3, HEAD, LANES), F32), VMEM((32, cols), F32), VMEM((32, cols), F32)]
        + [dma((steps, 3)), dma((3,)), dma((steps,)), dma((steps,))],
        input_output_aliases={3 + len(pieces): 0} if n_prev else {},
        compiler_params=pltpu.CompilerParams(vmem_limit_bytes=VMEM_BYTES),
        cost_estimate=pl.CostEstimate(flops=10**5, bytes_accessed=8 * 10**6, transcendentals=0),
        name="mix",
    )(mix, stat, logits, *pieces, *([prev] if n_prev else []))


CHUNKS = (6144, 10240)


def solution(mesh):
    store_devs = mesh.shape["store"]
    model_devs = mesh.shape["model"]
    assert store_devs == 2 and model_devs == 4
    group_axes = ("store", "model")
    across_y = [(0, 1), (1, 0)]
    across_core = [(0, 1), (1, 0), (2, 3), (3, 2)]
    across_x = [(0, 2), (2, 0), (1, 3), (3, 1)]

    def swap_y(value):
        return lax.ppermute(value, "store", across_y)

    def swap_core(value):
        return lax.ppermute(value, "model", across_core)

    def swap_x(value):
        return lax.ppermute(value, "model", across_x)

    def local_step(queries, w_head, store_keys, store_tok, temperature, mix_weight):
        vocab = w_head.shape[1] * model_devs
        tau = temperature.reshape(1)
        mix = mix_weight.reshape(1)

        their_tok = swap_y(store_tok)
        own, first, second = [], [], []
        start = 0
        for index, count in enumerate(CHUNKS):
            joined = index == 0
            kept, *sent = score_call(tau, queries, store_keys, start, count, joined)
            own.append(kept)
            first.append(swap_y(sent[0]))
            if joined:
                second.append(first[-1])
            else:
                second.append(swap_y(sent[1]))
            start += count

        kept = histogram_call(store_tok, None, own, [], None, vocab)
        nears, fars = [], []
        after = kept[0]
        for index, parts in enumerate((first, second)):
            out = histogram_call(their_tok, index, parts, kept[index::2], after, vocab)
            far = swap_core(out[0])
            near = swap_core(out[2])
            sums = merge_call(out[1], far, index == 1)
            if index == 0:
                after = sums[0]
                fars.append([swap_x(sums[0])])
            else:
                fars.append([swap_x(sums[0])])
            nears.append([out[3], near])
        logits, stat = head_call(queries, w_head, sums[0])
        for swap in (swap_core, swap_x):
            other = swap(stat)
            top = jnp.maximum(stat[0], other[0])
            stat = jnp.stack([top, stat[1] * jnp.exp(stat[0] - top) + other[1] * jnp.exp(other[0] - top)])
        fars[1].append(swap_x(sums[1]))
        result = None
        for index in range(2):
            result = mix_call(mix, nears[index] + fars[index], logits, stat, index, result)
        return result

    return jax.shard_map(
        local_step,
        mesh=mesh,
        in_specs=(P("data", None), P(None, "model"), P(group_axes, None), P(group_axes), P(), P()),
        out_specs=P(("data", "store"), "model"),
        check_vma=False,
    )
```

```python
import functools

import jax
import jax.numpy as jnp
from jax import lax
from jax.experimental import pallas as pl
from jax.experimental.pallas import tpu as pltpu
from jax.sharding import PartitionSpec as P


F32 = jnp.float32
ANY = pl.ANY
VMEM = pltpu.VMEM
SMEM = pltpu.SMEM
KEY_BLOCK = 1024
LANES = 128
VMEM_BYTES = 67043328
BATCH_KEYS = 8
FLAG_KEYS = 32
STEP_ROWS = 4
PACK = 4
TOK_BLOCK = 128
ORDERS = ((0, 2, 1, 3), (3, 0, 2, 1))
STAGE_BLOCKS = 5
HEAD = 8


def lane_group(width):
    return lax.broadcasted_iota(jnp.int32, (1, LANES), 1) // width


def pick(group, parts):
    out = parts[-1]
    for index in range(len(parts) - 2, -1, -1):
        out = jnp.where(group == index, parts[index], out)
    return out


def roll(value, shift):
    return pltpu.roll(value, shift % LANES, 1)


def score_kernel(tau_ref, rows_ref, k_ref, own_ref, *sent):
    *sent, q_ref = sent
    tau = tau_ref[0]
    first_ref, second_ref = (sent[0].at[0], sent[0].at[1]) if len(sent) == 1 else sent

    @pl.when(pl.program_id(0) == 0)
    def _():
        half = q_ref.shape[0] // 2
        y = lax.axis_index("store")
        q_ref[0:half, :] = rows_ref[pl.ds(pl.multiple_of(y * half, half), half), :]
        q_ref[half : 2 * half, :] = rows_ref[pl.ds(pl.multiple_of((1 - y) * half, half), half), :]

    dots = lax.dot_general(k_ref[...], q_ref[...], (((1,), (1,)), ((), ())), preferred_element_type=F32)
    step = LANES
    norms = []
    for row in range(0, KEY_BLOCK, step):
        acc = jnp.zeros((step, LANES), F32)
        for col in range(0, k_ref.shape[1], LANES):
            part = k_ref[row : row + step, col : col + LANES].astype(F32)
            acc += part * part
        norms.append(jnp.sum(acc, axis=1, keepdims=True))
    group = lane_group(32)
    scores = [(2.0 * dots[i * step : (i + 1) * step] - norms[i]) / tau for i in range(KEY_BLOCK // step)]
    for i in range(KEY_BLOCK // step // 2):
        own_ref[i * step : (i + 1) * step, :] = jnp.where(group < 2, scores[2 * i], roll(scores[2 * i + 1], 64))
    for i in range(KEY_BLOCK // step // 4):
        four = scores[4 * i : 4 * i + 4]
        rows = slice(i * step, (i + 1) * step)
        first_ref[rows, :] = pick(group, [roll(four[0], 64), roll(four[1], 96), four[2], roll(four[3], 32)])
        second_ref[rows, :] = pick(group, [roll(four[0], 32), roll(four[1], 64), roll(four[2], 96), four[3]])


def score_call(tau, queries, keys, start, count, joined):
    width = keys.shape[1]
    base = start // KEY_BLOCK
    half, quarter = KEY_BLOCK // 2, KEY_BLOCK // 4
    if joined:
        sent_shape = (jax.ShapeDtypeStruct((2, count // 4, LANES), F32),)
        sent_spec = (pl.BlockSpec((2, quarter, LANES), lambda i: (0, i, 0)),)
    else:
        sent_shape = (jax.ShapeDtypeStruct((count // 4, LANES), F32),) * 2
        sent_spec = (pl.BlockSpec((quarter, LANES), lambda i: (i, 0)),) * 2
    return pl.pallas_call(
        score_kernel,
        grid=(count // KEY_BLOCK,),
        out_shape=(jax.ShapeDtypeStruct((count // 2, LANES), F32),) + sent_shape,
        in_specs=[
            pl.BlockSpec(memory_space=SMEM),
            pl.BlockSpec((LANES, width), lambda i: (0, 0)),
            pl.BlockSpec((KEY_BLOCK, width), lambda i: (i + base, 0)),
        ],
        out_specs=(pl.BlockSpec((half, LANES), lambda i: (i, 0)),) + sent_spec,
        scratch_shapes=[VMEM((LANES, width), jnp.bfloat16)],
        compiler_params=pltpu.CompilerParams(vmem_limit_bytes=VMEM_BYTES),
        cost_estimate=pl.CostEstimate(flops=2 * count * width * LANES, bytes_accessed=2 * count * width, transcendentals=0),
        name="scores",
    )(tau, queries, keys)


def place_ids(tok_ref, which, group_ref, ids_ref, line_ref, flag_ref, sem):
    assert PACK == 4 and TOK_BLOCK == LANES
    tok = tok_ref[...]
    block, run, within = tok >> 9, (tok >> 7) & 3, tok & 127
    if which is None:
        line = block * 256 + (run >> 1) * LANES + within
        group = run & 1
    else:
        line = block * LANES + within
        group = sum(jnp.where(run == ORDERS[which][g], g, 0) for g in range(PACK))
    lane = lax.broadcasted_iota(jnp.int32, (1, LANES), 1)
    meet = jnp.zeros(tok.shape, F32)
    for shift in range(1, BATCH_KEYS):
        same = (line == roll(line, shift)) & (lane % BATCH_KEYS >= shift)
        meet = jnp.where(same, 1.0, meet)
    rows = lax.broadcasted_iota(jnp.int32, (LANES, LANES), 0) // FLAG_KEYS
    shared = (rows == lax.broadcasted_iota(jnp.int32, (LANES, LANES), 1) // FLAG_KEYS).astype(F32)
    ids_ref[0] = line
    ids_ref[1] = jnp.dot(meet, shared, preferred_element_type=F32).astype(jnp.int32)
    group_ref[...] = group.astype(F32).T.astype(jnp.bfloat16)
    return [
        pltpu.make_async_copy(ids_ref.at[0], line_ref, sem.at[0]),
        pltpu.make_async_copy(ids_ref.at[1], flag_ref, sem.at[1]),
    ]


def load_parts(parts, which, scores, sem):
    copies = []
    start = 0
    for i, part in enumerate(parts):
        part = part.at[which] if len(part.shape) == 3 else part
        copies.append(pltpu.make_async_copy(part, scores.at[pl.ds(start, part.shape[0])], sem.at[i]))
        copies[-1].start()
        start += part.shape[0]
    return copies


def clear(hist):
    step = 512

    def body(i, carry):
        hist[pl.ds(pl.multiple_of(i * step, step), step), :] = jnp.zeros((step, LANES), F32)
        return carry

    lax.fori_loop(0, hist.shape[0] // step, body, 0)


def across(value, width, combine):
    while width < LANES:
        value = combine(value, roll(value, width))
        width *= 2
    return value


def top_of(scores, width):
    step = 512

    def body(i, best):
        block = scores[pl.ds(pl.multiple_of(i * step, step), step), :]
        return jnp.maximum(best, jnp.max(block.reshape(step // 8, 8, LANES), axis=0))

    best = lax.fori_loop(0, scores.shape[0] // step, body, jnp.full((8, LANES), -jnp.inf, F32))
    return across(jnp.max(best, axis=0, keepdims=True), width, jnp.maximum)


def spread_weights(scores, weights, group_ref, top, width):
    count = LANES // width
    group = lane_group(width)
    spread_lane = lax.broadcasted_iota(jnp.int32, (LANES, LANES), 1) // width
    spread_row = lax.broadcasted_iota(jnp.int32, (LANES, LANES), 0)
    together = 4

    def body(i, total):
        for u in range(together):
            block = i * together + u
            select = (spread_row == block * count + spread_lane).astype(F32).astype(jnp.bfloat16)
            target = jnp.dot(group_ref[...], select, preferred_element_type=F32).astype(jnp.int32)
            shift = (target - group) & (count - 1)
            value = jnp.exp(scores[pl.ds(pl.multiple_of(block * LANES, LANES), LANES), :] - top)
            total = total + jnp.sum(value.reshape(16, 8, LANES), axis=0)
            turned = [jnp.where(shift == d, value, 0.0) for d in range(count)]
            turned = [turned[0]] + [roll(turned[d], width * d) for d in range(1, count)]
            for source in range(count):
                line = pick(group, [turned[(g - source) % count] for g in range(count)])
                at = pl.multiple_of((block * count + source) * LANES, LANES)
                weights[pl.ds(at, LANES), :] = line
        return total

    total = lax.fori_loop(0, scores.shape[0] // LANES // together, body, jnp.zeros((8, LANES), F32))
    return across(jnp.sum(total, axis=0, keepdims=True), width, jnp.add)


def add_weights(line_ref, flag_ref, weights, hists):
    def add(hist, row, lane, key, count):
        at = [line_ref[row, lane + k] for k in range(count)]
        sums = [hist[pl.ds(at[k], 1), :] + weights[pl.ds(key + k, 1), :] for k in range(count)]
        for k in range(count):
            hist[pl.ds(at[k], 1), :] = sums[k]

    def body(i, carry):
        first = i * STEP_ROWS
        groups = [(r, lane) for r in range(STEP_ROWS) for lane in range(0, LANES, FLAG_KEYS)]
        flags = [flag_ref[first + r, lane] for r, lane in groups]

        def apart(r, lane, count):
            for b in range(count // BATCH_KEYS):
                at = lane + b * BATCH_KEYS
                add(hists[b % 2], first + r, at, (first + r) * LANES + at, BATCH_KEYS)

        def one_by_one(r, lane):
            def step(k, carry):
                for which in range(2):
                    at = lane + 2 * k + which
                    add(hists[which], first + r, at, (first + r) * LANES + at, 1)
                return carry

            lax.fori_loop(0, FLAG_KEYS // 2, step, 0)

        def all_apart():
            for r in range(STEP_ROWS):
                apart(r, 0, LANES)

        def some_apart():
            for (r, lane), flag in zip(groups, flags):
                lax.cond(flag == 0, lambda: apart(r, lane, FLAG_KEYS), lambda: one_by_one(r, lane))

        lax.cond(sum(flags) == 0, all_apart, some_apart)
        return carry

    lax.fori_loop(0, weights.shape[0] // LANES // STEP_ROWS, body, 0)


def piece_at(k, size):
    model = lax.axis_index("model")
    x, core = model // 2, model % 2
    x_of = x if k >= 2 else 1 - x
    core_of = core if k % 2 else 1 - core
    return (2 * x_of + core_of) * size


def head_block(top, total):
    row = lax.broadcasted_iota(jnp.int32, (HEAD, LANES), 0)
    return jnp.where(row == 0, top, jnp.where(row == 1, total, 0.0))


def own_kernel(which, n_parts, tok_ref, *refs):
    parts, refs = refs[:n_parts], refs[n_parts:]
    outs, refs = refs[:8], refs[8:]
    group_ref, ids_ref, line_ref, flag_ref, id_sem, scores, weights, even, odd, heads, in_sem, out_sem, head_sem = refs
    lines = even.shape[0]
    piece = lines // 8
    copies = load_parts(parts, which, scores, in_sem)
    copies += place_ids(tok_ref, which, group_ref, ids_ref, line_ref, flag_ref, id_sem)
    for copy in copies[-2:]:
        copy.start()
    clear(even)
    clear(odd)
    for copy in copies:
        copy.wait()
    top = top_of(scores, 64)
    total = spread_weights(scores, weights, group_ref, top, 64)
    add_weights(line_ref, flag_ref, weights, (even, odd))

    quad = lane_group(32) % 2 == 0
    tops = [jnp.where(quad, top, roll(top, 32)), jnp.where(quad, roll(top, 32), top)]
    totals = [jnp.where(quad, total, roll(total, 32)), jnp.where(quad, roll(total, 32), total)]
    for c in range(2):
        heads[c] = head_block(tops[c], totals[c])
    together = 5

    sends = []
    for k in range(4):
        base = piece_at(k, 1)

        def split(i, carry, base=base):
            values = []
            for u in range(together):
                block = i * together + u
                near = pl.ds(pl.multiple_of(base * 2 * piece + block * 256, LANES), LANES)
                far = pl.ds(pl.multiple_of(base * 2 * piece + block * 256 + LANES, LANES), LANES)
                low = even[near, :] + odd[near, :]
                high = roll(even[far, :] + odd[far, :], 32)
                values.append((block, low, high))
            for block, low, high in values:
                weights[pl.ds(pl.multiple_of(base * piece + block * LANES, LANES), LANES), :] = jnp.where(quad, low, high)
                even[pl.ds(pl.multiple_of(base * 2 * piece + block * LANES, LANES), LANES), :] = jnp.where(quad, high, low)
            return carry

        lax.fori_loop(0, piece // LANES // together, split, 0)
        firsts = weights.at[pl.ds(pl.multiple_of(base * piece, LANES), piece)]
        seconds = even.at[pl.ds(pl.multiple_of(base * 2 * piece, LANES), piece)]
        for c, source in enumerate((firsts, seconds)):
            out = outs[k * 2 + c]
            sends.append(pltpu.make_async_copy(source, out.at[pl.ds(0, piece)], out_sem.at[c, k]))
            sends.append(pltpu.make_async_copy(heads.at[c], out.at[pl.ds(piece, HEAD)], head_sem.at[c, k]))
        for send in sends[-4:]:
            send.start()
    for send in sends:
        send.wait()


def chunk_kernel(which, n_parts, tok_ref, *refs):
    parts, refs = refs[:n_parts], refs[n_parts:]
    prevs, refs = refs[:4], refs[5:]
    outs, refs = refs[:4], refs[4:]
    group_ref, ids_ref, line_ref, flag_ref, id_sem, scores, weights, even, odd, heads, in_sem, *refs = refs
    held, prev_sem, out_sem, head_sem = refs
    lines = even.shape[0]
    piece = lines // 4
    copies = load_parts(parts, which, scores, in_sem)
    fetches = [pltpu.make_async_copy(prevs[k], held.at[k], prev_sem.at[k]) for k in range(4)]
    for fetch in fetches:
        fetch.start()
    copies += place_ids(tok_ref, which, group_ref, ids_ref, line_ref, flag_ref, id_sem)
    for copy in copies[-2:]:
        copy.start()
    clear(even)
    clear(odd)
    for copy in copies:
        copy.wait()
    top = top_of(scores, 32)
    total = spread_weights(scores, weights, group_ref, top, 32)
    add_weights(line_ref, flag_ref, weights, (even, odd))

    for fetch in fetches:
        fetch.wait()
    old_top, old_total = held[0, piece : piece + 1, :], held[0, piece + 1 : piece + 2, :]
    new_top = jnp.maximum(top, old_top)
    scale, old_scale = jnp.exp(top - new_top), jnp.exp(old_top - new_top)
    heads[0] = head_block(new_top, total * scale + old_total * old_scale)
    step = LANES
    sends = []
    for k in range(4):
        base = piece_at(k, piece)

        def join(i, carry, base=base, k=k):
            at = pl.ds(pl.multiple_of(base + i * step, step), step)
            old = held[k, pl.ds(pl.multiple_of(i * step, step), step), :]
            even[at, :] = (even[at, :] + odd[at, :]) * scale + old * old_scale
            return carry

        lax.fori_loop(0, piece // step, join, 0)
        source = even.at[pl.ds(pl.multiple_of(base, step), piece)]
        sends.append(pltpu.make_async_copy(source, outs[k].at[pl.ds(0, piece)], out_sem.at[k]))
        sends.append(pltpu.make_async_copy(heads.at[0], outs[k].at[pl.ds(piece, HEAD)], head_sem.at[k]))
        for send in sends[-2:]:
            send.start()
    for send in sends:
        send.wait()


def histogram_call(tok, which, parts, prevs, after, vocab):
    own = not prevs
    rows = sum(part.shape[-2] for part in parts)
    lines = vocab // (2 if own else PACK)
    out = jax.ShapeDtypeStruct((vocab // PACK // 4 + HEAD, LANES), F32)
    keys = tok.shape[0]
    tok = tok.reshape(LANES, LANES)
    assert keys == LANES * LANES
    count = 8 if own else 4
    dma = pltpu.SemaphoreType.DMA
    extra = [] if own else [*prevs, after]
    return pl.pallas_call(
        functools.partial(own_kernel if own else chunk_kernel, which, len(parts)),
        out_shape=(out,) * count,
        in_specs=[pl.BlockSpec(memory_space=VMEM)]
        + [pl.BlockSpec(memory_space=ANY)] * (len(parts) + len(extra)),
        out_specs=(pl.BlockSpec(memory_space=ANY),) * count,
        scratch_shapes=[VMEM((LANES, LANES), jnp.bfloat16), VMEM((2, LANES, LANES), jnp.int32)]
        + [SMEM((LANES, LANES), jnp.int32), SMEM((LANES, LANES), jnp.int32), dma((2,))]
        + [VMEM((rows, LANES), F32), VMEM((keys, LANES), F32), VMEM((lines, LANES), F32), VMEM((lines, LANES), F32)]
        + [VMEM((2, HEAD, LANES), F32), dma((len(parts),))]
        + ([dma((2, 4)), dma((2, 4))] if own else [VMEM((4, lines // 4 + HEAD, LANES), F32), dma((4,)), dma((4,)), dma((4,))]),
        compiler_params=pltpu.CompilerParams(vmem_limit_bytes=VMEM_BYTES),
        cost_estimate=pl.CostEstimate(flops=10**6, bytes_accessed=2 * 10**7, transcendentals=0),
        name="own_histogram" if own else "chunk_histogram",
    )(tok, *parts, *extra)


def merge_kernel(a_ref, b_ref, *refs):
    *outs, a_held, b_held, heads, in_sem, out_sem = refs
    lines = a_ref.shape[0] - HEAD
    block = STAGE_BLOCKS * TOK_BLOCK
    steps = lines // block

    def fetch(source, held, which, start, size, index):
        at = pl.ds(start, size)
        return pltpu.make_async_copy(source.at[at], held.at[at], in_sem.at[which, index])

    pairs = [(lines, HEAD)] + [(i * block, block) for i in range(steps)]
    fetches = [
        (fetch(a_ref, a_held, 0, start, size, i), fetch(b_ref, b_held, 1, start, size, i))
        for i, (start, size) in enumerate(pairs)
    ]
    for pair in fetches:
        for copy in pair:
            copy.start()
    sends = []
    for i, (start, size) in enumerate(pairs):
        for copy in fetches[i]:
            copy.wait()
        if i == 0:
            a_top, b_top = a_held[lines : lines + 1, :], b_held[lines : lines + 1, :]
            top = jnp.maximum(a_top, b_top)
            a_scale, b_scale = jnp.exp(a_top - top), jnp.exp(b_top - top)
            total = a_held[lines + 1 : lines + 2, :] * a_scale + b_held[lines + 1 : lines + 2, :] * b_scale
            heads[...] = head_block(top, total)
            source = heads
        else:
            at = slice(start, start + size)
            a_held[at, :] = a_held[at, :] * a_scale + b_held[at, :] * b_scale
            source = a_held.at[pl.ds(start, size)]
        if len(outs) == 1:
            target = outs[0].at[pl.ds(start, size)]
        else:
            first = outs[0].shape[0]
            target = outs[0].at[pl.ds(start, size)] if start < first else outs[1].at[pl.ds(start - first, size)]
        sends.append(pltpu.make_async_copy(source, target, out_sem.at[i]))
        sends[-1].start()
    for send in sends:
        send.wait()


def merge_call(a, b, parted):
    block = STAGE_BLOCKS * TOK_BLOCK
    steps = a.shape[0] // block
    sizes = (a.shape[0] - HEAD - block, block + HEAD) if parted else (a.shape[0],)
    dma = pltpu.SemaphoreType.DMA
    return pl.pallas_call(
        merge_kernel,
        out_shape=tuple(jax.ShapeDtypeStruct((size, LANES), F32) for size in sizes),
        in_specs=[pl.BlockSpec(memory_space=ANY)] * 2,
        out_specs=tuple(pl.BlockSpec(memory_space=ANY) for _ in sizes),
        scratch_shapes=[VMEM(a.shape, F32), VMEM(a.shape, F32), VMEM((HEAD, LANES), F32), dma((2, steps + 1)), dma((steps + 1,))],
        compiler_params=pltpu.CompilerParams(vmem_limit_bytes=VMEM_BYTES),
        cost_estimate=pl.CostEstimate(flops=10**5, bytes_accessed=3 * a.size * 4, transcendentals=0),
        name="merge",
    )(a, b)


def head_kernel(q_ref, w_ref, after_ref, logits_ref, stat_ref, top_ref, sum_ref):
    del after_ref
    i = pl.program_id(0)

    @pl.when(i == 0)
    def _():
        top_ref[...] = jnp.full(top_ref.shape, -jnp.inf, F32)
        sum_ref[...] = jnp.zeros(sum_ref.shape, F32)

    rows = logits_ref.shape[0]
    mine = q_ref[pl.ds(pl.multiple_of(lax.axis_index("store") * rows, rows), rows), :]
    logits = jnp.dot(mine, w_ref[...], preferred_element_type=F32)
    logits_ref[...] = logits
    old = top_ref[...]
    new = jnp.maximum(old, jnp.max(logits, axis=1, keepdims=True))
    part = jnp.sum(jnp.exp(logits - new[:, 0:1]), axis=1, keepdims=True)
    sum_ref[...] = sum_ref[...] * jnp.exp(old - new) + part
    top_ref[...] = new
    stat_ref[0] = top_ref[...]
    stat_ref[1] = sum_ref[...]


def head_call(queries, w_head, after):
    width = queries.shape[1]
    count = queries.shape[0] // 2
    cols = w_head.shape[1]
    block = cols // 10
    return pl.pallas_call(
        head_kernel,
        grid=(cols // block,),
        out_shape=(jax.ShapeDtypeStruct((count, cols), F32), jax.ShapeDtypeStruct((2, count, LANES), F32)),
        in_specs=[
            pl.BlockSpec((2 * count, width), lambda i: (0, 0)),
            pl.BlockSpec((width, block), lambda i: (0, i)),
            pl.BlockSpec(memory_space=ANY),
        ],
        out_specs=(pl.BlockSpec((count, block), lambda i: (0, i)), pl.BlockSpec((2, count, LANES), lambda i: (0, 0, 0))),
        scratch_shapes=[VMEM((count, LANES), F32), VMEM((count, LANES), F32)],
        compiler_params=pltpu.CompilerParams(vmem_limit_bytes=VMEM_BYTES),
        cost_estimate=pl.CostEstimate(flops=2 * count * width * cols, bytes_accessed=2 * width * cols, transcendentals=0),
        name="head",
    )(queries, w_head, after)


def mix_kernel(index, n_far, n_prev, mix_ref, stat_ref, logits_ref, *refs):
    pieces, refs = refs[: 2 + n_far], refs[2 + n_far + n_prev :]
    out_ref, held, heads, logits, result, in_sem, head_sem, logits_sem, out_sem = refs
    order = ORDERS[index]
    block = STAGE_BLOCKS * TOK_BLOCK
    steps = held.shape[1] // block
    wide = block * PACK
    rows = pl.ds(index * 32, 32)

    def sources(start, size):
        first = pieces[2].shape[0]
        far = pieces[2].at[pl.ds(start, size)] if start < first else pieces[3].at[pl.ds(start - first, size)]
        return [pieces[0].at[pl.ds(start, size)], pieces[1].at[pl.ds(start, size)], far]

    head_copies = [
        pltpu.make_async_copy(source, heads.at[p], head_sem.at[p])
        for p, source in enumerate(sources(steps * block, HEAD))
    ]
    for copy in head_copies:
        copy.start()
    copies = []
    for i in range(steps):
        at = pl.ds(i * block, block)
        cols = pl.ds(i * wide, wide)
        group = [
            pltpu.make_async_copy(source, held.at[p, at], in_sem.at[i, p])
            for p, source in enumerate(sources(i * block, block))
        ]
        group.append(pltpu.make_async_copy(logits_ref.at[rows, cols], logits.at[:, cols], logits_sem.at[i]))
        for copy in group:
            copy.start()
        copies.append(group)
    for copy in head_copies:
        copy.wait()
    mix = mix_ref[0]
    tops = [heads[p, 0:1, :] for p in range(3)]
    top = jnp.maximum(jnp.maximum(tops[0], tops[1]), tops[2])
    scales = [jnp.exp(value - top) for value in tops]
    total = sum(heads[p, 1:2, :] * scales[p] for p in range(3))
    scales = [scale * mix / total for scale in scales]
    lm_top = stat_ref[0, index * 32 : index * 32 + 32, :]
    lm_scale = (1.0 - mix) / stat_ref[1, index * 32 : index * 32 + 32, :]
    sends = []
    for i in range(steps):
        for copy in copies[i]:
            copy.wait()
        for b in range(i * STAGE_BLOCKS, (i + 1) * STAGE_BLOCKS):
            at = slice(b * TOK_BLOCK, (b + 1) * TOK_BLOCK)
            turned = sum(held[p, at, :] * scales[p] for p in range(3)).T
            for g in range(PACK):
                run = order[g]
                cols = slice((b * PACK + run) * TOK_BLOCK, (b * PACK + run + 1) * TOK_BLOCK)
                lm = jnp.exp(logits[:, cols] - lm_top) * lm_scale
                result[:, cols] = jnp.log(turned[g * 32 : (g + 1) * 32, :] + lm)
        cols = pl.ds(i * wide, wide)
        sends.append(pltpu.make_async_copy(result.at[:, cols], out_ref.at[rows, cols], out_sem.at[i]))
        sends[-1].start()
    for send in sends:
        send.wait()


def mix_call(mix, pieces, logits, stat, index, prev):
    lines = pieces[0].shape[0] - HEAD
    steps = lines // (STAGE_BLOCKS * TOK_BLOCK)
    count, cols = logits.shape
    n_prev = 0 if prev is None else 1
    dma = pltpu.SemaphoreType.DMA
    return pl.pallas_call(
        functools.partial(mix_kernel, index, len(pieces) - 2, n_prev),
        out_shape=jax.ShapeDtypeStruct((count, cols), F32),
        in_specs=[pl.BlockSpec(memory_space=SMEM), pl.BlockSpec(memory_space=VMEM)]
        + [pl.BlockSpec(memory_space=ANY)] * (1 + len(pieces) + n_prev),
        out_specs=pl.BlockSpec(memory_space=ANY),
        scratch_shapes=[VMEM((3, lines, LANES), F32), VMEM((3, HEAD, LANES), F32), VMEM((32, cols), F32), VMEM((32, cols), F32)]
        + [dma((steps, 3)), dma((3,)), dma((steps,)), dma((steps,))],
        input_output_aliases={3 + len(pieces): 0} if n_prev else {},
        compiler_params=pltpu.CompilerParams(vmem_limit_bytes=VMEM_BYTES),
        cost_estimate=pl.CostEstimate(flops=10**5, bytes_accessed=8 * 10**6, transcendentals=0),
        name="mix",
    )(mix, stat, logits, *pieces, *([prev] if n_prev else []))


CHUNKS = (5120, 11264)


def solution(mesh):
    store_devs = mesh.shape["store"]
    model_devs = mesh.shape["model"]
    assert store_devs == 2 and model_devs == 4
    group_axes = ("store", "model")
    across_y = [(0, 1), (1, 0)]
    across_core = [(0, 1), (1, 0), (2, 3), (3, 2)]
    across_x = [(0, 2), (2, 0), (1, 3), (3, 1)]

    def swap_y(value):
        return lax.ppermute(value, "store", across_y)

    def swap_core(value):
        return lax.ppermute(value, "model", across_core)

    def swap_x(value):
        return lax.ppermute(value, "model", across_x)

    def local_step(queries, w_head, store_keys, store_tok, temperature, mix_weight):
        vocab = w_head.shape[1] * model_devs
        tau = temperature.reshape(1)
        mix = mix_weight.reshape(1)

        their_tok = swap_y(store_tok)
        own, first, second = [], [], []
        start = 0
        for index, count in enumerate(CHUNKS):
            joined = index == 0
            kept, *sent = score_call(tau, queries, store_keys, start, count, joined)
            own.append(kept)
            first.append(swap_y(sent[0]))
            if joined:
                second.append(first[-1])
            else:
                second.append(swap_y(sent[1]))
            start += count

        kept = histogram_call(store_tok, None, own, [], None, vocab)
        nears, fars = [], []
        after = kept[0]
        for index, parts in enumerate((first, second)):
            out = histogram_call(their_tok, index, parts, kept[index::2], after, vocab)
            far = swap_core(out[0])
            near = swap_core(out[2])
            sums = merge_call(out[1], far, index == 1)
            if index == 0:
                after = sums[0]
                fars.append([swap_x(sums[0])])
            else:
                fars.append([swap_x(sums[0])])
            nears.append([out[3], near])
        logits, stat = head_call(queries, w_head, sums[0])
        for swap in (swap_core, swap_x):
            other = swap(stat)
            top = jnp.maximum(stat[0], other[0])
            stat = jnp.stack([top, stat[1] * jnp.exp(stat[0] - top) + other[1] * jnp.exp(other[0] - top)])
        fars[1].append(swap_x(sums[1]))
        result = None
        for index in range(2):
            result = mix_call(mix, nears[index] + fars[index], logits, stat, index, result)
        return result

    return jax.shard_map(
        local_step,
        mesh=mesh,
        in_specs=(P("data", None), P(None, "model"), P(group_axes, None), P(group_axes), P(), P()),
        out_specs=P(("data", "store"), "model"),
        check_vma=False,
    )
```
